256 devices in a mesh: dp: 128 (over y, z, x), mp: 2 (over core).
Axes of the slice: x: 4, y: 4, z: 8, core: 2. Of those that a mesh axis runs over, the one named last changes fastest.
Arguments:
- grad: bfloat16 [32, 1024, 8192], P(None, 'dp', 'mp'), may hold values from -6 to 6
- second_moment: float32 [32, 1024, 8192], P(None, 'dp', 'mp'), may hold values from 0.004 to 20, as said below
- left_root: bfloat16 [2, 128, 1024, 1024], P('mp', 'dp'), as said below
- right_root: bfloat16 [2, 128, 1024, 1024], P('mp', 'dp'), as said below
- owner_slot: int32 [2, 32, 4], replicated, may hold values from 0 to 127, as said below
Outputs:
- update: bfloat16 [32, 1024, 8192], P(None, 'dp', 'mp')
The draws below stay inside these ranges and needn't reach their ends.
Inputs may be any that keep to these rules, and one draw needn't show every extreme that they name: For each h, owner_slot[h] lists every dp index exactly once: each dp index owns one block of each h. `second_moment`: positive. `left_root`: each square is symmetric positive definite. `right_root`: each square is symmetric positive definite.
All inputs are finite; a program needn't handle non-finite values.
Results may differ from the reference program's by a relative error of at most 0.0049.
Values may be sent and summed in bfloat16 or wider, within the bound.
No kernel may reach another device: no remote copies, remote signals or barrier semaphores. Data moves between devices by JAX's collectives and lax.ppermute only.
A program may use at most 64 MiB of HBM per device.

```python
import jax
import jax.numpy as jnp
from jax import lax

D = 8192
BS = 1024
RB = 32
DH = 4096
CBH = 4
N_DP = 128
N_MP = 2


def draw_second_moment(key, part):
    key_rows, key_cols, key_elem = jax.random.split(jax.random.fold_in(key, 7), 3)
    position = jnp.arange(BS, dtype=jnp.float32) / (BS - 1)
    row_scale = jnp.exp(jax.random.uniform(key_rows, (RB, BS, 1), jnp.float32, jnp.log(0.3), jnp.log(3.0)))
    col_scale = jnp.exp(jax.random.uniform(key_cols, (RB, 1, D), jnp.float32, jnp.log(0.3), jnp.log(3.0)))
    trend = 3.0 ** (-position)
    element = jnp.exp(jax.random.uniform(key_elem, (RB, BS, D), jnp.float32, jnp.log(0.5), jnp.log(2.0)))
    return row_scale * col_scale * element * trend[None, :, None]


def root_square(key):
    key_diag, key_noise = jax.random.split(key)
    noise = jax.random.normal(key_noise, (BS, BS), jnp.float32)
    diagonal = jnp.exp(jax.random.uniform(key_diag, (BS,), jnp.float32, jnp.log(0.5), jnp.log(2.0)))
    spread = 0.2 / jnp.sqrt(2.0 * BS)
    return (noise + noise.T) * spread + jnp.diag(diagonal)


def root_stack(key):
    count = N_MP * N_DP
    keys = jax.random.split(key, count)
    squares = lax.map(root_square, keys)
    return squares.reshape(N_MP, N_DP, BS, BS)


def draw_left_root(key, part):
    return root_stack(jax.random.fold_in(key, 11)).astype(jnp.bfloat16)


def draw_right_root(key, part):
    return root_stack(jax.random.fold_in(key, 23)).astype(jnp.bfloat16)


def draw_owner_slot(key, part):
    halves = []
    for half_idx in range(N_MP):
        key_owner = jax.random.fold_in(key, 101 + half_idx)
        owners = jax.random.permutation(key_owner, N_DP).astype(jnp.int32)
        halves.append(owners.reshape(RB, CBH))
    return jnp.stack(halves).astype(jnp.int32)


def levels(own_key, dims, cuts, low, high):
    level = 1.0
    for dim, blocks in cuts:
        heights = jax.random.uniform(jax.random.fold_in(jax.random.fold_in(own_key, 6), dim), (blocks,), jnp.float32, low / len(cuts), high / len(cuts))
        level = level * jnp.repeat(jnp.exp(heights), dims[dim] // blocks).reshape((-1,) + (1,) * (len(dims) - 1 - dim))
    return level


def gaussian(own_key, shape, width, most, pieces=(), kind=jnp.bfloat16):
    result = jax.random.normal(own_key, shape, jnp.float32) * width
    if len(pieces) > 0:
        result = levels(own_key, shape, pieces, -0.22, 0.18) * result
    return jnp.clip(result, min=-most, max=most).astype(kind)


def setup_inputs(seed: int = 0) -> dict:
    arg_keys = jax.random.split(jax.random.key(seed), 6)
    return {
        "grad": gaussian(arg_keys[0], (RB, BS, D), 1.0, 6.0, ((1, 128), (2, 2))),
        "second_moment": draw_second_moment(jax.random.fold_in(arg_keys[5], 71), 0),
        "left_root": draw_left_root(jax.random.fold_in(arg_keys[5], 71), 0),
        "right_root": draw_right_root(jax.random.fold_in(arg_keys[5], 71), 0),
        "owner_slot": draw_owner_slot(jax.random.fold_in(arg_keys[5], 71), 0),
    }


BETA_TWO = 0.99
ADAM_EPS = 1e-08
NORM_EPS = 1e-06

def reference(grad, second_moment, left_root, right_root, owner_slot):
    widened = grad.astype(jnp.float32)
    moment_new = BETA_TWO * second_moment + (1.0 - BETA_TWO) * widened * widened
    direction = widened / (jnp.sqrt(moment_new) + ADAM_EPS)
    squares = lax.optimization_barrier(jnp.sum((direction * direction).reshape(RB, BS, N_MP, CBH, BS), axis=(1, 4)))

    def single(index):
        half_idx = index // (RB * CBH)
        row_idx = index // CBH % RB
        col_idx = index % CBH
        start = (half_idx * DH + col_idx * BS).astype(jnp.int32)
        block = lax.dynamic_slice(grad, (row_idx.astype(jnp.int32), jnp.int32(0), start), (1, BS, BS))[0]
        slot = owner_slot[half_idx, row_idx, col_idx]
        left = left_root[half_idx, slot]
        right = right_root[half_idx, slot]
        mixed = jnp.dot(block, right, preferred_element_type=jnp.float32).astype(jnp.bfloat16)
        shaped = jnp.dot(left, mixed, preferred_element_type=jnp.float32)
        shaped_sq = jnp.sum(shaped * shaped)
        adam_sq = squares[row_idx, half_idx, col_idx]
        factor = jnp.sqrt((adam_sq + NORM_EPS) / (shaped_sq + NORM_EPS))
        return (shaped * factor).astype(jnp.bfloat16)
    results = lax.map(single, jnp.arange(N_MP * RB * CBH, dtype=jnp.int32))
    results = results.reshape(N_MP, RB, CBH, BS, BS).transpose(1, 3, 0, 2, 4)
    return results.reshape(RB, BS, D)
```

```python
import functools

import jax
import jax.numpy as jnp
from jax import lax
from jax.experimental import pallas as pl
from jax.experimental.pallas import tpu as pltpu
from jax.sharding import Mesh
from jax.sharding import PartitionSpec as P

DP = ("dp_0", "dp_1", "dp_2")


BETA_TWO = 0.99
ADAM_EPS = 1e-08
NORM_EPS = 1e-06
MIB = 1 << 20


def gather_kernel(groups, table_ref, grad_ref, out_ref, held_ref, in_sem, out_sem):
    row_blocks = grad_ref.shape[0]
    block_size = out_ref.shape[-1]
    col_blocks = grad_ref.shape[2] // block_size
    group = row_blocks // groups
    base = lax.axis_index("mp") * (row_blocks * col_blocks)

    def load(g):
        rows = pl.ds(g * group, group)
        return pltpu.make_async_copy(grad_ref.at[rows], held_ref.at[rows], in_sem.at[g])

    for g in range(groups):
        load(g).start()
    for g in range(groups):
        load(g).wait()

        def one_row(row, carry):
            for col in range(col_blocks):
                slot = table_ref[base + row * col_blocks + col]
                pltpu.make_async_copy(
                    held_ref.at[row, :, pl.ds(col * block_size, block_size)], out_ref.at[slot], out_sem
                ).start()
            return carry

        lax.fori_loop(g * group, (g + 1) * group, one_row, 0)
    pltpu.make_async_copy(out_ref, out_ref, out_sem).wait()


def scatter_kernel(table_ref, back_ref, out_ref, sem):
    row_blocks = out_ref.shape[0]
    block_size = back_ref.shape[-1]
    col_blocks = out_ref.shape[2] // block_size
    base = lax.axis_index("mp") * (row_blocks * col_blocks)

    def one_row(row, carry):
        for col in range(col_blocks):
            slot = table_ref[base + row * col_blocks + col]
            pltpu.make_async_copy(
                back_ref.at[slot], out_ref.at[row, :, pl.ds(col * block_size, block_size)], sem
            ).start()
        return carry

    lax.fori_loop(0, row_blocks, one_row, 0)
    pltpu.make_async_copy(out_ref, out_ref, sem).wait()


def block_kernel(parts, tile, table_ref, *refs):
    part_refs = refs[:parts]
    rows_hbm, right_hbm, left_hbm, out_ref, rows_ref, right_ref, left_ref, mixed_ref, shaped_ref, sem = refs[parts:]
    block_size = right_hbm.shape[0]
    steps = block_size // tile

    def rows_load(i):
        rows = pl.ds(i * tile, tile)
        return pltpu.make_async_copy(rows_hbm.at[rows], rows_ref.at[rows], sem.at[i])

    def right_load(i):
        cols = pl.ds(i * tile, tile)
        return pltpu.make_async_copy(right_hbm.at[:, cols], right_ref.at[:, cols], sem.at[steps + i])

    left_load = pltpu.make_async_copy(left_hbm, left_ref, sem.at[2 * steps])
    right_load(0).start()
    for i in range(steps):
        rows_load(i).start()
    for i in range(1, steps):
        right_load(i).start()
    left_load.start()
    me = lax.axis_index(DP)
    totals = part_refs[0][...]
    for part_ref in part_refs[1:]:
        totals = totals + part_ref[...]
    adam_sq = jnp.sum(jnp.where(table_ref[...] == me, totals, 0.0))
    for j in range(steps):
        cols = pl.ds(j * tile, tile)
        right_load(j).wait()
        for i in range(steps):
            rows = pl.ds(i * tile, tile)
            if j == 0:
                rows_load(i).wait()
            mixed_ref[rows, cols] = jnp.dot(
                rows_ref[rows, :], right_ref[:, cols], preferred_element_type=jnp.float32
            ).astype(jnp.bfloat16)
    left_load.wait()
    squares = jnp.zeros((8, tile), jnp.float32)
    for i in range(steps):
        cols = pl.ds(i * tile, tile)
        shaped = jnp.dot(left_ref[...], mixed_ref[:, cols], preferred_element_type=jnp.float32)
        shaped_ref[:, cols] = shaped
        squares = squares + jnp.sum((shaped * shaped).reshape(block_size // 8, 8, tile), axis=0)
    shaped_sq = jnp.sum(squares)
    factor = jnp.sqrt(jnp.full((8, 128), adam_sq + NORM_EPS, jnp.float32) / (shaped_sq + NORM_EPS))
    scale = factor[0:1, 0:1]
    out_ref[...] = (shaped_ref[...] * scale).astype(jnp.bfloat16)


def per_device(grad, second_moment, left_root, right_root, owner_slot):
    row_blocks, block_rows, half_cols = grad.shape
    block_size = left_root.shape[-1]
    col_blocks = half_cols // block_size
    blocks = row_blocks * col_blocks
    dp_count = lax.axis_size(DP)
    mp_index = lax.axis_index("mp")
    table = owner_slot.reshape(-1)
    vmem = pl.BlockSpec(memory_space=pltpu.VMEM)
    hbm = pl.BlockSpec(memory_space=pltpu.HBM)
    smem = pl.BlockSpec(memory_space=pltpu.SMEM)
    square = jax.ShapeDtypeStruct((block_size, block_size), jnp.bfloat16)
    groups = 4

    def in_hbm(value):
        return pltpu.with_memory_space_constraint(value, pltpu.HBM)

    outgoing = pl.pallas_call(
        functools.partial(gather_kernel, groups),
        out_shape=jax.ShapeDtypeStruct((dp_count, block_rows, block_size), jnp.bfloat16),
        in_specs=[smem, hbm],
        out_specs=hbm,
        scratch_shapes=[
            pltpu.VMEM(grad.shape, jnp.bfloat16),
            pltpu.SemaphoreType.DMA((groups,)),
            pltpu.SemaphoreType.DMA,
        ],
        name="gather_rows",
    )(table, grad)
    rows_in = lax.all_to_all(outgoing, DP, split_axis=0, concat_axis=0, tiled=True)

    widened = grad.astype(jnp.float32)
    moment_new = BETA_TWO * second_moment + (1.0 - BETA_TWO) * widened * widened
    direction = widened / (jnp.sqrt(moment_new) + ADAM_EPS)
    partial_value = jnp.sum(
        (direction * direction).reshape(row_blocks, block_rows, col_blocks, block_size), axis=(1, 3)
    ).reshape(1, blocks)
    plane = lax.psum(lax.psum(partial_value, "dp_0"), "dp_2")
    depth = lax.axis_size("dp_1")
    parts = [plane]
    for step in range(1, depth):
        ring = [(i, (i + step) % depth) for i in range(depth)]
        parts.append(lax.ppermute(plane, "dp_1", ring))
    half_table = lax.dynamic_index_in_dim(owner_slot, mp_index, 0, keepdims=False).reshape(1, blocks)

    tile = block_size // 4
    result = pl.pallas_call(
        functools.partial(block_kernel, depth, tile),
        out_shape=square,
        in_specs=[vmem] * (depth + 1) + [hbm] * 3,
        out_specs=vmem,
        scratch_shapes=[
            pltpu.VMEM((block_size, block_size), jnp.bfloat16),
            pltpu.VMEM((block_size, block_size), jnp.bfloat16),
            pltpu.VMEM((block_size, block_size), jnp.bfloat16),
            pltpu.VMEM((block_size, block_size), jnp.bfloat16),
            pltpu.VMEM((block_size, block_size), jnp.float32),
            pltpu.SemaphoreType.DMA((2 * (block_size // tile) + 1,)),
        ],
        compiler_params=pltpu.CompilerParams(vmem_limit_bytes=24 * MIB),
        name="own_block",
        cost_estimate=pl.CostEstimate(
            flops=4 * block_size**3, bytes_accessed=8 * block_size**2, transcendentals=0
        ),
    )(half_table, *parts, in_hbm(rows_in.reshape(block_size, block_size)), in_hbm(right_root[0, 0]), in_hbm(left_root[0, 0]))

    back = lax.all_to_all(
        result.reshape(dp_count, block_rows, block_size), DP, split_axis=0, concat_axis=0, tiled=True
    )
    return pl.pallas_call(
        scatter_kernel,
        out_shape=jax.ShapeDtypeStruct(grad.shape, jnp.bfloat16),
        in_specs=[smem, vmem],
        out_specs=hbm,
        scratch_shapes=[pltpu.SemaphoreType.DMA],
        compiler_params=pltpu.CompilerParams(vmem_limit_bytes=8 * MIB),
        name="scatter_rows",
    )(table, back)


def solution(mesh):
    split = Mesh(mesh.devices.reshape(4, 8, 4, mesh.shape["mp"]), ("dp_0", "dp_1", "dp_2", "mp"))
    return jax.shard_map(
        per_device,
        mesh=split,
        in_specs=(
            P(None, DP, "mp"),
            P(None, DP, "mp"),
            P("mp", DP, None, None),
            P("mp", DP, None, None),
            P(),
        ),
        out_specs=P(None, DP, "mp"),
        check_vma=False,
    )
```

```python
import functools

import jax
import jax.numpy as jnp
from jax import lax
from jax.experimental import pallas as pl
from jax.experimental.pallas import tpu as pltpu
from jax.sharding import Mesh
from jax.sharding import PartitionSpec as P

DP = ("dp_0", "dp_1", "dp_2")


BETA_TWO = 0.99
ADAM_EPS = 1e-08
NORM_EPS = 1e-06
MIB = 1 << 20
VMEM = pl.BlockSpec(memory_space=pltpu.VMEM)
HBM = pl.BlockSpec(memory_space=pltpu.HBM)
SMEM = pl.BlockSpec(memory_space=pltpu.SMEM)


def in_hbm(value):
    return pltpu.with_memory_space_constraint(value, pltpu.HBM)


def gather_kernel(groups, half, table_ref, grad_ref, out_ref, held_ref, in_sem, out_sem):
    row_blocks = grad_ref.shape[0]
    block_size = out_ref.shape[-1]
    col_blocks = grad_ref.shape[2] // block_size
    group = row_blocks // groups

    def load(g):
        rows = pl.ds(g * group, group)
        return pltpu.make_async_copy(grad_ref.at[rows], held_ref.at[rows], in_sem.at[g])

    for g in range(groups):
        load(g).start()
    for g in range(groups):
        load(g).wait()

        def one_row(row, carry):
            for col in range(col_blocks):
                pltpu.make_async_copy(
                    held_ref.at[row, :, pl.ds(col * block_size, block_size)],
                    out_ref.at[table_ref[half, col, row]],
                    out_sem,
                ).start()
            return carry

        lax.fori_loop(g * group, (g + 1) * group, one_row, 0)
    pltpu.make_async_copy(out_ref, out_ref, out_sem).wait()


def gather_rows(table, grad, half, slots, block_size):
    groups = 4
    return pl.pallas_call(
        functools.partial(gather_kernel, groups, half),
        out_shape=pltpu.HBM((slots, grad.shape[1], block_size), jnp.bfloat16),
        in_specs=[SMEM, HBM],
        out_specs=HBM,
        scratch_shapes=[
            pltpu.VMEM(grad.shape, jnp.bfloat16),
            pltpu.SemaphoreType.DMA((groups,)),
            pltpu.SemaphoreType.DMA,
        ],
        name="gather_rows",
    )(table, grad)


def scatter_kernel(half, table_ref, back_ref, out_ref, sem):
    row_blocks = out_ref.shape[0]
    block_size = back_ref.shape[-1]
    col_blocks = out_ref.shape[2] // block_size

    def one_row(row, carry):
        for col in range(col_blocks):
            pltpu.make_async_copy(
                back_ref.at[table_ref[half, col, row]],
                out_ref.at[row, :, pl.ds(col * block_size, block_size)],
                sem,
            ).start()
        return carry

    lax.fori_loop(0, row_blocks, one_row, 0)
    pltpu.make_async_copy(out_ref, out_ref, sem).wait()


def scaled_scatter_kernel(parts, half, table_ref, *refs):
    part_refs = refs[:parts]
    back_ref, out_ref, norm_ref, held_ref, sem = refs[parts:]
    row_blocks = out_ref.shape[0]
    block_size = back_ref.shape[-1]
    col_blocks = out_ref.shape[2] // block_size
    blocks = row_blocks * col_blocks
    totals = part_refs[0][...]
    for part_ref in part_refs[1:]:
        totals = totals + part_ref[...]
    norms = jnp.sqrt(totals + NORM_EPS)
    norm_ref[...] = jnp.transpose(jnp.broadcast_to(norms, (blocks, blocks)))

    def one_row(row, carry):
        for col in range(col_blocks):
            slot = table_ref[half, col, row]
            norm = norm_ref[pl.ds(row * col_blocks + col, 1), :]
            norm = jnp.concatenate([norm] * (block_size // blocks), axis=1)
            rows = back_ref[slot].astype(jnp.float32) * norm
            held_ref[row, :, pl.ds(col * block_size, block_size)] = rows.astype(jnp.bfloat16)
        pltpu.make_async_copy(held_ref.at[row], out_ref.at[row], sem).start()
        return carry

    lax.fori_loop(0, row_blocks, one_row, 0)
    pltpu.make_async_copy(out_ref, out_ref, sem).wait()


def scatter_rows(table, back, half, like, parts=None):
    out_shape = pltpu.HBM(like.shape, jnp.bfloat16)
    params = pltpu.CompilerParams(vmem_limit_bytes=8 * MIB)
    if parts is None:
        return pl.pallas_call(
            functools.partial(scatter_kernel, half),
            out_shape=out_shape,
            in_specs=[SMEM, VMEM],
            out_specs=HBM,
            scratch_shapes=[pltpu.SemaphoreType.DMA],
            compiler_params=params,
            name="scatter_rows",
        )(table, back)
    blocks = parts[0].shape[1]
    return pl.pallas_call(
        functools.partial(scaled_scatter_kernel, len(parts), half),
        out_shape=out_shape,
        in_specs=[SMEM] + [VMEM] * (len(parts) + 1),
        out_specs=HBM,
        scratch_shapes=[
            pltpu.VMEM((blocks, blocks), jnp.float32),
            pltpu.VMEM(like.shape, jnp.bfloat16),
            pltpu.SemaphoreType.DMA,
        ],
        compiler_params=params,
        name="scaled_scatter_rows",
    )(table, *parts, back)


def block_kernel(parts, tile, *refs):
    if parts > 0:
        table_ref, part_refs, refs = refs[0], refs[1 : 1 + parts], refs[1 + parts :]
    rows_hbm, right_hbm, left_hbm, out_hbm, rows_ref, right_ref, left_ref, mixed_ref, shaped_ref, out_ref, sem = refs
    block_size = right_hbm.shape[0]
    steps = block_size // tile

    def rows_load(i):
        rows = pl.ds(i * tile, tile)
        return pltpu.make_async_copy(rows_hbm.at[rows], rows_ref.at[rows], sem.at[i])

    def right_load(i):
        cols = pl.ds(i * tile, tile)
        return pltpu.make_async_copy(right_hbm.at[:, cols], right_ref.at[:, cols], sem.at[steps + i])

    def store(i):
        rows = pl.ds(i * tile, tile)
        return pltpu.make_async_copy(out_ref.at[rows], out_hbm.at[rows], sem.at[i])

    left_load = pltpu.make_async_copy(left_hbm, left_ref, sem.at[2 * steps])
    right_load(0).start()
    for i in range(steps):
        rows_load(i).start()
    for i in range(1, steps):
        right_load(i).start()
    left_load.start()
    adam_sq = None
    if parts > 0:
        totals = part_refs[0][...]
        for part_ref in part_refs[1:]:
            totals = totals + part_ref[...]
        adam_sq = jnp.sum(jnp.where(table_ref[...] == lax.axis_index(DP), totals, 0.0))
    for i in range(steps):
        rows_load(i).wait()

    def mix(j, carry):
        cols = pl.ds(pl.multiple_of(j * tile, tile), tile)
        right_load(j).wait()
        mixed_ref[:, cols] = jnp.dot(
            rows_ref[...], right_ref[:, cols], preferred_element_type=jnp.float32
        ).astype(jnp.bfloat16)
        return carry

    lax.fori_loop(0, steps, mix, 0)
    left_load.wait()

    def shape(j, squares):
        cols = pl.ds(pl.multiple_of(j * tile, tile), tile)
        shaped = jnp.dot(left_ref[...], mixed_ref[:, cols], preferred_element_type=jnp.float32)
        shaped_ref[:, cols] = shaped
        return squares + jnp.sum((shaped * shaped).reshape(block_size // 8, 8, tile), axis=0)

    squares = lax.fori_loop(0, steps, shape, jnp.zeros((8, tile), jnp.float32))
    shaped_sq = jnp.full((8, 128), jnp.sum(squares), jnp.float32)
    if parts > 0:
        factor = jnp.sqrt((adam_sq + NORM_EPS) / (shaped_sq + NORM_EPS))
    else:
        factor = 1.0 / jnp.sqrt(shaped_sq + NORM_EPS)
    scale = factor[0:1, 0:1]

    def finish(i, carry):
        rows = pl.ds(pl.multiple_of(i * tile, tile), tile)
        out_ref[rows, :] = (shaped_ref[rows, :] * scale).astype(jnp.bfloat16)
        store(i).start()
        return carry

    lax.fori_loop(0, steps, finish, 0)
    for i in range(steps):
        store(i).wait()


def own_block(rows_in, right, left, table=None, parts=()):
    block_size = right.shape[0]
    tile = block_size // 4
    square = pltpu.VMEM((block_size, block_size), jnp.bfloat16)
    small = () if table is None else (table, *parts)
    return pl.pallas_call(
        functools.partial(block_kernel, len(parts), tile),
        out_shape=pltpu.HBM((block_size, block_size), jnp.bfloat16),
        in_specs=[VMEM] * len(small) + [HBM] * 3,
        out_specs=HBM,
        scratch_shapes=[
            square,
            square,
            square,
            square,
            pltpu.VMEM((block_size, block_size), jnp.float32),
            square,
            pltpu.SemaphoreType.DMA((2 * (block_size // tile) + 1,)),
        ],
        compiler_params=pltpu.CompilerParams(vmem_limit_bytes=32 * MIB),
        name="own_block",
        cost_estimate=pl.CostEstimate(
            flops=4 * block_size**3, bytes_accessed=8 * block_size**2, transcendentals=0
        ),
    )(*small, in_hbm(rows_in), in_hbm(right), in_hbm(left))


def exchange(value):
    return lax.all_to_all(value, DP, split_axis=0, concat_axis=0, tiled=True)


def plane_sums(grad, second_moment, block_size):
    row_blocks, block_rows, half_cols = grad.shape
    col_blocks = half_cols // block_size
    widened = grad.astype(jnp.float32)
    moment_new = BETA_TWO * second_moment + (1.0 - BETA_TWO) * widened * widened
    direction = widened / (jnp.sqrt(moment_new) + ADAM_EPS)
    partial_value = jnp.sum(
        (direction * direction).reshape(row_blocks, block_rows, col_blocks, block_size), axis=(1, 3)
    ).reshape(1, row_blocks * col_blocks)
    return lax.psum(lax.psum(partial_value, "dp_0"), "dp_2")


def all_planes(plane):
    depth = lax.axis_size("dp_1")
    parts = [plane]
    for step in range(1, depth):
        ring = [(i, (i + step) % depth) for i in range(depth)]
        parts.append(lax.ppermute(plane, "dp_1", ring))
    return parts


def first_core(grad, second_moment, left, right, table):
    block_size = left.shape[0]
    slots = lax.axis_size(DP)
    outgoing = gather_rows(table, grad, 0, slots, block_size)
    rows_in = exchange(outgoing)
    plane = plane_sums(grad, second_moment, block_size)
    result = own_block(rows_in.reshape(block_size, block_size), right, left)
    plane, result = lax.optimization_barrier((plane, result))
    back = exchange(result.reshape(outgoing.shape))
    return scatter_rows(table, back, 0, grad, all_planes(plane))


def second_core(grad, second_moment, left, right, table):
    block_size = left.shape[0]
    slots = lax.axis_size(DP)
    outgoing = gather_rows(table, grad, 1, slots, block_size)
    plane = plane_sums(grad, second_moment, block_size)
    plane, outgoing = lax.optimization_barrier((plane, outgoing))
    rows_in = exchange(outgoing)
    own_table = jnp.transpose(table[1]).reshape(1, -1)
    result = own_block(
        rows_in.reshape(block_size, block_size), right, left, own_table, all_planes(plane)
    )
    back = exchange(result.reshape(outgoing.shape))
    return scatter_rows(table, back, 1, grad)


def per_device(grad, second_moment, left_root, right_root, owner_slot):
    table = jnp.transpose(owner_slot, (0, 2, 1))
    return lax.cond(
        lax.axis_index("mp") == 0,
        first_core,
        second_core,
        grad,
        second_moment,
        left_root[0, 0],
        right_root[0, 0],
        table,
    )


def solution(mesh):
    split = Mesh(mesh.devices.reshape(4, 8, 4, mesh.shape["mp"]), ("dp_0", "dp_1", "dp_2", "mp"))
    return jax.shard_map(
        per_device,
        mesh=split,
        in_specs=(
            P(None, DP, "mp"),
            P(None, DP, "mp"),
            P("mp", DP, None, None),
            P("mp", DP, None, None),
            P(),
        ),
        out_specs=P(None, DP, "mp"),
        check_vma=False,
    )
```

```python
import functools

import jax
import jax.numpy as jnp
from jax import lax
from jax.experimental import pallas as pl
from jax.experimental.pallas import tpu as pltpu
from jax.sharding import Mesh
from jax.sharding import PartitionSpec as P

DP = ("dp_0", "dp_1", "dp_2")


BETA_TWO = 0.99
ADAM_EPS = 1e-08
NORM_EPS = 1e-06
MIB = 1 << 20
VMEM = pl.BlockSpec(memory_space=pltpu.VMEM)
HBM = pl.BlockSpec(memory_space=pltpu.HBM)
SMEM = pl.BlockSpec(memory_space=pltpu.SMEM)


def in_hbm(value):
    return pltpu.with_memory_space_constraint(value, pltpu.HBM)


def gather_kernel(groups, half, table_hbm, grad_ref, out_ref, table_ref, held_ref, table_sem, in_sem, out_sem):
    row_blocks = grad_ref.shape[0]
    block_size = out_ref.shape[-1]
    col_blocks = grad_ref.shape[2] // block_size
    group = row_blocks // groups

    def load(g):
        rows = pl.ds(g * group, group)
        return pltpu.make_async_copy(grad_ref.at[rows], held_ref.at[rows], in_sem.at[g])

    table_load = pltpu.make_async_copy(table_hbm, table_ref, table_sem)
    table_load.start()
    for g in range(groups):
        load(g).start()
    table_load.wait()
    for g in range(groups):
        load(g).wait()

        def one_row(row, carry):
            for col in range(col_blocks):
                pltpu.make_async_copy(
                    held_ref.at[row, :, pl.ds(col * block_size, block_size)],
                    out_ref.at[table_ref[half, col, row]],
                    out_sem,
                ).start()
            return carry

        lax.fori_loop(g * group, (g + 1) * group, one_row, 0)
    pltpu.make_async_copy(out_ref, out_ref, out_sem).wait()


def gather_rows(table, grad, half, slots, block_size):
    groups = 8
    return pl.pallas_call(
        functools.partial(gather_kernel, groups, half),
        out_shape=pltpu.HBM((slots, grad.shape[1], block_size), jnp.bfloat16),
        in_specs=[HBM, HBM],
        out_specs=HBM,
        scratch_shapes=[
            pltpu.SMEM(table.shape, jnp.int32),
            pltpu.VMEM(grad.shape, jnp.bfloat16),
            pltpu.SemaphoreType.DMA,
            pltpu.SemaphoreType.DMA((groups,)),
            pltpu.SemaphoreType.DMA,
        ],
        name="gather_rows",
    )(in_hbm(table), in_hbm(grad))


def scatter_kernel(half, table_ref, back_ref, out_ref, sem):
    row_blocks = out_ref.shape[0]
    block_size = back_ref.shape[-1]
    col_blocks = out_ref.shape[2] // block_size

    def one_row(row, carry):
        for col in range(col_blocks):
            pltpu.make_async_copy(
                back_ref.at[table_ref[half, col, row]],
                out_ref.at[row, :, pl.ds(col * block_size, block_size)],
                sem,
            ).start()
        return carry

    lax.fori_loop(0, row_blocks, one_row, 0)
    pltpu.make_async_copy(out_ref, out_ref, sem).wait()


def scaled_scatter_kernel(parts, half, table_ref, *refs):
    part_refs = refs[:parts]
    back_ref, out_ref, norm_ref, held_ref, sem = refs[parts:]
    row_blocks = out_ref.shape[0]
    block_size = back_ref.shape[-1]
    col_blocks = out_ref.shape[2] // block_size
    blocks = row_blocks * col_blocks
    totals = part_refs[0][...]
    for part_ref in part_refs[1:]:
        totals = totals + part_ref[...]
    norms = jnp.sqrt(totals + NORM_EPS)
    norm_ref[...] = jnp.transpose(jnp.broadcast_to(norms, (blocks, blocks)))

    def one_row(row, carry):
        for col in range(col_blocks):
            slot = table_ref[half, col, row]
            norm = norm_ref[pl.ds(row * col_blocks + col, 1), :]
            norm = jnp.concatenate([norm] * (block_size // blocks), axis=1)
            rows = back_ref[slot].astype(jnp.float32) * norm
            held_ref[row, :, pl.ds(col * block_size, block_size)] = rows.astype(jnp.bfloat16)
        pltpu.make_async_copy(held_ref.at[row], out_ref.at[row], sem).start()
        return carry

    lax.fori_loop(0, row_blocks, one_row, 0)
    pltpu.make_async_copy(out_ref, out_ref, sem).wait()


def scatter_rows(table, back, half, like, parts=None):
    out_shape = pltpu.HBM(like.shape, jnp.bfloat16)
    params = pltpu.CompilerParams(vmem_limit_bytes=8 * MIB)
    if parts is None:
        return pl.pallas_call(
            functools.partial(scatter_kernel, half),
            out_shape=out_shape,
            in_specs=[SMEM, VMEM],
            out_specs=HBM,
            scratch_shapes=[pltpu.SemaphoreType.DMA],
            compiler_params=params,
            name="scatter_rows",
        )(table, back)
    blocks = parts[0].shape[1]
    return pl.pallas_call(
        functools.partial(scaled_scatter_kernel, len(parts), half),
        out_shape=out_shape,
        in_specs=[SMEM] + [VMEM] * (len(parts) + 1),
        out_specs=HBM,
        scratch_shapes=[
            pltpu.VMEM((blocks, blocks), jnp.float32),
            pltpu.VMEM(like.shape, jnp.bfloat16),
            pltpu.SemaphoreType.DMA,
        ],
        compiler_params=params,
        name="scaled_scatter_rows",
    )(table, *parts, back)


def block_kernel(parts, tile, *refs):
    if parts > 0:
        table_ref, part_refs, refs = refs[0], refs[1 : 1 + parts], refs[1 + parts :]
    rows_ref, right_hbm, left_hbm, out_ref, right_ref, left_ref, mixed_ref, shaped_ref, sem = refs[:9]
    block_size = right_hbm.shape[0]
    steps = block_size // tile

    def right_load(i):
        cols = pl.ds(i * tile, tile)
        return pltpu.make_async_copy(right_hbm.at[:, cols], right_ref.at[:, cols], sem.at[i])

    left_load = pltpu.make_async_copy(left_hbm, left_ref, sem.at[steps])
    for i in range(steps):
        right_load(i).start()
    left_load.start()
    adam_sq = None
    if parts > 0:
        totals = part_refs[0][...]
        for part_ref in part_refs[1:]:
            totals = totals + part_ref[...]
        adam_sq = jnp.sum(jnp.where(table_ref[...] == lax.axis_index(DP), totals, 0.0))

    def mix(j, carry):
        cols = pl.ds(pl.multiple_of(j * tile, tile), tile)
        right_load(j).wait()
        mixed_ref[:, cols] = jnp.dot(
            rows_ref[...], right_ref[:, cols], preferred_element_type=jnp.float32
        ).astype(jnp.bfloat16)
        return carry

    lax.fori_loop(0, steps, mix, 0)
    left_load.wait()

    def shape(j, squares):
        cols = pl.ds(pl.multiple_of(j * tile, tile), tile)
        shaped = jnp.dot(left_ref[...], mixed_ref[:, cols], preferred_element_type=jnp.float32)
        shaped_ref[:, cols] = shaped
        return squares + jnp.sum((shaped * shaped).reshape(block_size // 8, 8, tile), axis=0)

    squares = lax.fori_loop(0, steps, shape, jnp.zeros((8, tile), jnp.float32))
    shaped_sq = jnp.full((8, 128), jnp.sum(squares), jnp.float32)
    if parts > 0:
        factor = jnp.sqrt((adam_sq + NORM_EPS) / (shaped_sq + NORM_EPS))
    else:
        factor = 1.0 / jnp.sqrt(shaped_sq + NORM_EPS)
    scale = factor[0:1, 0:1]
    band = block_size // 4

    if len(refs) == 9:

        def finish(i, carry):
            rows = pl.ds(pl.multiple_of(i * band, band), band)
            out_ref[rows, :] = (shaped_ref[rows, :] * scale).astype(jnp.bfloat16)
            return carry

        lax.fori_loop(0, 4, finish, 0)
    else:
        held_ref = refs[9]

        def finish(i, carry):
            rows = pl.ds(pl.multiple_of(i * band, band), band)
            held_ref[rows, :] = (shaped_ref[rows, :] * scale).astype(jnp.bfloat16)
            pltpu.make_async_copy(held_ref.at[rows], out_ref.at[rows], sem.at[0]).start()
            return carry

        lax.fori_loop(0, 4, finish, 0)
        pltpu.make_async_copy(held_ref, out_ref, sem.at[0]).wait()


def own_block(rows_in, right, left, out_in_hbm, table=None, parts=()):
    block_size = right.shape[0]
    tile = block_size // 2
    square = pltpu.VMEM((block_size, block_size), jnp.bfloat16)
    small = () if table is None else (table, *parts)
    shape = (block_size, block_size)
    return pl.pallas_call(
        functools.partial(block_kernel, len(parts), tile),
        out_shape=pltpu.HBM(shape, jnp.bfloat16) if out_in_hbm else jax.ShapeDtypeStruct(shape, jnp.bfloat16),
        in_specs=[VMEM] * (len(small) + 1) + [HBM] * 2,
        out_specs=HBM if out_in_hbm else VMEM,
        scratch_shapes=[
            square,
            square,
            square,
            pltpu.VMEM(shape, jnp.float32),
            pltpu.SemaphoreType.DMA((block_size // tile + 1,)),
        ]
        + [square] * out_in_hbm,
        compiler_params=pltpu.CompilerParams(vmem_limit_bytes=24 * MIB),
        name="own_block",
        cost_estimate=pl.CostEstimate(
            flops=4 * block_size**3, bytes_accessed=8 * block_size**2, transcendentals=0
        ),
    )(*small, rows_in, in_hbm(right), in_hbm(left))


def exchange(value):
    return lax.all_to_all(value, DP, split_axis=0, concat_axis=0, tiled=True)


def plane_sums(grad, second_moment, block_size):
    row_blocks, block_rows, half_cols = grad.shape
    col_blocks = half_cols // block_size
    widened = grad.astype(jnp.float32)
    moment_new = BETA_TWO * second_moment + (1.0 - BETA_TWO) * widened * widened
    direction = widened / (jnp.sqrt(moment_new) + ADAM_EPS)
    partial_value = jnp.sum(
        (direction * direction).reshape(row_blocks, block_rows, col_blocks, block_size), axis=(1, 3)
    ).reshape(1, row_blocks * col_blocks)
    return lax.psum(lax.psum(partial_value, "dp_0"), "dp_2")


def all_planes(plane):
    depth = lax.axis_size("dp_1")
    parts = [plane]
    for step in range(1, depth):
        ring = [(i, (i + step) % depth) for i in range(depth)]
        parts.append(lax.ppermute(plane, "dp_1", ring))
    return parts


def first_core(grad, second_moment, left, right, table):
    block_size = left.shape[0]
    slots = lax.axis_size(DP)
    outgoing = gather_rows(table, grad, 0, slots, block_size)
    rows_in = exchange(outgoing)
    plane = plane_sums(grad, second_moment, block_size)
    result = own_block(rows_in.reshape(block_size, block_size), right, left, True)
    plane, result = lax.optimization_barrier((plane, result))
    back = exchange(result.reshape(outgoing.shape))
    return scatter_rows(table, back, 0, grad, all_planes(plane))


def second_core(grad, second_moment, left, right, table):
    block_size = left.shape[0]
    slots = lax.axis_size(DP)
    outgoing = gather_rows(table, grad, 1, slots, block_size)
    plane = plane_sums(grad, second_moment, block_size)
    plane, outgoing = lax.optimization_barrier((plane, outgoing))
    rows_in = exchange(outgoing)
    own_table = jnp.transpose(table[1]).reshape(1, -1)
    result = own_block(
        rows_in.reshape(block_size, block_size), right, left, False, own_table, all_planes(plane)
    )
    back = exchange(result.reshape(outgoing.shape))
    return scatter_rows(table, back, 1, grad)


def per_device(grad, second_moment, left_root, right_root, owner_slot):
    table = jnp.transpose(owner_slot, (0, 2, 1))
    return lax.cond(
        lax.axis_index("mp") == 0,
        first_core,
        second_core,
        grad,
        second_moment,
        left_root[0, 0],
        right_root[0, 0],
        table,
    )


def solution(mesh):
    split = Mesh(mesh.devices.reshape(4, 8, 4, mesh.shape["mp"]), ("dp_0", "dp_1", "dp_2", "mp"))
    return jax.shard_map(
        per_device,
        mesh=split,
        in_specs=(
            P(None, DP, "mp"),
            P(None, DP, "mp"),
            P("mp", DP, None, None),
            P("mp", DP, None, None),
            P(),
        ),
        out_specs=P(None, DP, "mp"),
        check_vma=False,
    )
```

```python
import functools

import jax
import jax.numpy as jnp
from jax import lax
from jax.experimental import pallas as pl
from jax.experimental.pallas import tpu as pltpu
from jax.sharding import Mesh
from jax.sharding import PartitionSpec as P

DP = ("dp_0", "dp_1", "dp_2")


BETA_TWO = 0.99
ADAM_EPS = 1e-08
NORM_EPS = 1e-06
MIB = 1 << 20
VMEM = pl.BlockSpec(memory_space=pltpu.VMEM)
HBM = pl.BlockSpec(memory_space=pltpu.HBM)
SMEM = pl.BlockSpec(memory_space=pltpu.SMEM)


def in_hbm(value):
    return pltpu.with_memory_space_constraint(value, pltpu.HBM)


def gather_kernel(groups, half, table_hbm, grad_ref, out_ref, table_ref, held_ref, table_sem, in_sem, out_sem):
    row_blocks = grad_ref.shape[0]
    block_size = out_ref.shape[-1]
    col_blocks = grad_ref.shape[2] // block_size
    group = row_blocks // groups

    def load(g):
        rows = pl.ds(g * group, group)
        return pltpu.make_async_copy(grad_ref.at[rows], held_ref.at[rows], in_sem.at[g])

    table_load = pltpu.make_async_copy(table_hbm, table_ref, table_sem)
    table_load.start()
    for g in range(groups):
        load(g).start()
    table_load.wait()
    for g in range(groups):
        load(g).wait()

        def one_row(row, carry):
            for col in range(col_blocks):
                pltpu.make_async_copy(
                    held_ref.at[row, :, pl.ds(col * block_size, block_size)],
                    out_ref.at[table_ref[half, col, row]],
                    out_sem,
                ).start()
            return carry

        lax.fori_loop(g * group, (g + 1) * group, one_row, 0)
    pltpu.make_async_copy(out_ref, out_ref, out_sem).wait()


def gather_rows(table, grad, half, slots, block_size):
    groups = 8
    return pl.pallas_call(
        functools.partial(gather_kernel, groups, half),
        out_shape=pltpu.HBM((slots, grad.shape[1], block_size), jnp.bfloat16),
        in_specs=[HBM, HBM],
        out_specs=HBM,
        scratch_shapes=[
            pltpu.SMEM(table.shape, jnp.int32),
            pltpu.VMEM(grad.shape, jnp.bfloat16),
            pltpu.SemaphoreType.DMA,
            pltpu.SemaphoreType.DMA((groups,)),
            pltpu.SemaphoreType.DMA,
        ],
        name="gather_rows",
    )(in_hbm(table), in_hbm(grad))


def scatter_kernel(half, table_ref, back_ref, out_ref, sem):
    row_blocks = out_ref.shape[0]
    block_size = back_ref.shape[-1]
    col_blocks = out_ref.shape[2] // block_size

    def one_row(row, carry):
        for col in range(col_blocks):
            pltpu.make_async_copy(
                back_ref.at[table_ref[half, col, row]],
                out_ref.at[row, :, pl.ds(col * block_size, block_size)],
                sem,
            ).start()
        return carry

    lax.fori_loop(0, row_blocks, one_row, 0)
    pltpu.make_async_copy(out_ref, out_ref, sem).wait()


def scaled_scatter_kernel(parts, half, table_ref, *refs):
    part_refs = refs[:parts]
    back_ref, out_ref, norm_ref, held_ref, sem = refs[parts:]
    row_blocks = out_ref.shape[0]
    block_size = back_ref.shape[-1]
    col_blocks = out_ref.shape[2] // block_size
    blocks = row_blocks * col_blocks
    totals = part_refs[0][...]
    for part_ref in part_refs[1:]:
        totals = totals + part_ref[...]
    norms = jnp.sqrt(totals + NORM_EPS)
    norm_ref[...] = jnp.transpose(jnp.broadcast_to(norms, (blocks, blocks)))

    def one_row(row, carry):
        for col in range(col_blocks):
            slot = table_ref[half, col, row]
            norm = norm_ref[pl.ds(row * col_blocks + col, 1), :]
            norm = jnp.concatenate([norm] * (block_size // blocks), axis=1)
            rows = back_ref[slot].astype(jnp.float32) * norm
            held_ref[row, :, pl.ds(col * block_size, block_size)] = rows.astype(jnp.bfloat16)
        pltpu.make_async_copy(held_ref.at[row], out_ref.at[row], sem).start()
        return carry

    lax.fori_loop(0, row_blocks, one_row, 0)
    pltpu.make_async_copy(out_ref, out_ref, sem).wait()


def scatter_rows(table, back, half, like, parts=None):
    out_shape = pltpu.HBM(like.shape, jnp.bfloat16)
    params = pltpu.CompilerParams(vmem_limit_bytes=8 * MIB)
    if parts is None:
        return pl.pallas_call(
            functools.partial(scatter_kernel, half),
            out_shape=out_shape,
            in_specs=[SMEM, VMEM],
            out_specs=HBM,
            scratch_shapes=[pltpu.SemaphoreType.DMA],
            compiler_params=params,
            name="scatter_rows",
        )(table, back)
    blocks = parts[0].shape[1]
    return pl.pallas_call(
        functools.partial(scaled_scatter_kernel, len(parts), half),
        out_shape=out_shape,
        in_specs=[SMEM] + [VMEM] * (len(parts) + 1),
        out_specs=HBM,
        scratch_shapes=[
            pltpu.VMEM((blocks, blocks), jnp.float32),
            pltpu.VMEM(like.shape, jnp.bfloat16),
            pltpu.SemaphoreType.DMA,
        ],
        compiler_params=params,
        name="scaled_scatter_rows",
    )(table, *parts, back)


def fetch_kernel(after_ref, right_hbm, out_ref, sem):
    columns = right_hbm.at[:, pl.ds(0, out_ref.shape[1])]
    copy = pltpu.make_async_copy(columns, out_ref, sem)
    copy.start()
    copy.wait()


def fetch_columns(after, right, columns):
    return pl.pallas_call(
        fetch_kernel,
        out_shape=jax.ShapeDtypeStruct((right.shape[0], columns), jnp.bfloat16),
        in_specs=[VMEM, HBM],
        out_specs=VMEM,
        scratch_shapes=[pltpu.SemaphoreType.DMA],
        compiler_params=pltpu.CompilerParams(vmem_limit_bytes=8 * MIB),
        name="fetch_columns",
    )(after, in_hbm(right))


def block_kernel(parts, tile, *refs):
    if parts > 0:
        table_ref, part_refs, refs = refs[0], refs[1 : 1 + parts], refs[1 + parts :]
    rows_ref, first_ref, right_hbm, left_hbm, out_ref, right_ref, left_ref, mixed_ref, shaped_ref, sem = refs[:10]
    block_size = right_hbm.shape[0]
    steps = block_size // tile

    def right_load(i):
        cols = pl.ds(i * tile, tile)
        return pltpu.make_async_copy(right_hbm.at[:, cols], right_ref.at[:, cols], sem.at[i])

    left_load = pltpu.make_async_copy(left_hbm, left_ref, sem.at[steps])
    for i in range(1, steps):
        right_load(i).start()
    left_load.start()
    adam_sq = None
    if parts > 0:
        totals = part_refs[0][...]
        for part_ref in part_refs[1:]:
            totals = totals + part_ref[...]
        adam_sq = jnp.sum(jnp.where(table_ref[...] == lax.axis_index(DP), totals, 0.0))

    for j in range(steps):
        cols = pl.ds(j * tile, tile)
        if j > 0:
            right_load(j).wait()
        columns = right_ref[:, cols] if j > 0 else first_ref[...]
        mixed_ref[:, cols] = jnp.dot(
            rows_ref[...], columns, preferred_element_type=jnp.float32
        ).astype(jnp.bfloat16)
    left_load.wait()

    def shape(j, squares):
        cols = pl.ds(pl.multiple_of(j * tile, tile), tile)
        shaped = jnp.dot(left_ref[...], mixed_ref[:, cols], preferred_element_type=jnp.float32)
        shaped_ref[:, cols] = shaped
        return squares + jnp.sum((shaped * shaped).reshape(block_size // 8, 8, tile), axis=0)

    squares = lax.fori_loop(0, steps, shape, jnp.zeros((8, tile), jnp.float32))
    shaped_sq = jnp.full((8, 128), jnp.sum(squares), jnp.float32)
    if parts > 0:
        factor = jnp.sqrt((adam_sq + NORM_EPS) / (shaped_sq + NORM_EPS))
    else:
        factor = 1.0 / jnp.sqrt(shaped_sq + NORM_EPS)
    scale = factor[0:1, 0:1]
    band = block_size // 4

    if len(refs) == 10:

        def finish(i, carry):
            rows = pl.ds(pl.multiple_of(i * band, band), band)
            out_ref[rows, :] = (shaped_ref[rows, :] * scale).astype(jnp.bfloat16)
            return carry

        lax.fori_loop(0, 4, finish, 0)
    else:
        held_ref = refs[10]

        def finish(i, carry):
            rows = pl.ds(pl.multiple_of(i * band, band), band)
            held_ref[rows, :] = (shaped_ref[rows, :] * scale).astype(jnp.bfloat16)
            pltpu.make_async_copy(held_ref.at[rows], out_ref.at[rows], sem.at[0]).start()
            return carry

        lax.fori_loop(0, 4, finish, 0)
        pltpu.make_async_copy(held_ref, out_ref, sem.at[0]).wait()


def own_block(rows_in, first, right, left, out_in_hbm, table=None, parts=()):
    block_size = right.shape[0]
    tile = first.shape[1]
    square = pltpu.VMEM((block_size, block_size), jnp.bfloat16)
    small = () if table is None else (table, *parts)
    shape = (block_size, block_size)
    return pl.pallas_call(
        functools.partial(block_kernel, len(parts), tile),
        out_shape=pltpu.HBM(shape, jnp.bfloat16) if out_in_hbm else jax.ShapeDtypeStruct(shape, jnp.bfloat16),
        in_specs=[VMEM] * (len(small) + 2) + [HBM] * 2,
        out_specs=HBM if out_in_hbm else VMEM,
        scratch_shapes=[
            square,
            square,
            square,
            pltpu.VMEM(shape, jnp.float32),
            pltpu.SemaphoreType.DMA((block_size // tile + 1,)),
        ]
        + [square] * out_in_hbm,
        compiler_params=pltpu.CompilerParams(vmem_limit_bytes=24 * MIB),
        name="own_block",
        cost_estimate=pl.CostEstimate(
            flops=4 * block_size**3, bytes_accessed=8 * block_size**2, transcendentals=0
        ),
    )(*small, rows_in, first, in_hbm(right), in_hbm(left))


def exchange(value):
    return lax.all_to_all(value, DP, split_axis=0, concat_axis=0, tiled=True)


def plane_sums(grad, second_moment, block_size):
    row_blocks, block_rows, half_cols = grad.shape
    col_blocks = half_cols // block_size
    widened = grad.astype(jnp.float32)
    moment_new = BETA_TWO * second_moment + (1.0 - BETA_TWO) * widened * widened
    direction = widened / (jnp.sqrt(moment_new) + ADAM_EPS)
    partial_value = jnp.sum(
        (direction * direction).reshape(row_blocks, block_rows, col_blocks, block_size), axis=(1, 3)
    ).reshape(1, row_blocks * col_blocks)
    return lax.psum(lax.psum(partial_value, "dp_0"), "dp_2")


def all_planes(plane):
    depth = lax.axis_size("dp_1")
    parts = [plane]
    for step in range(1, depth):
        ring = [(i, (i + step) % depth) for i in range(depth)]
        parts.append(lax.ppermute(plane, "dp_1", ring))
    return parts


def first_core(grad, second_moment, left, right, table):
    block_size = left.shape[0]
    slots = lax.axis_size(DP)
    outgoing = gather_rows(table, grad, 0, slots, block_size)
    rows_in = exchange(outgoing)
    plane = plane_sums(grad, second_moment, block_size)
    first = fetch_columns(plane, right, block_size // 2)
    result = own_block(rows_in.reshape(block_size, block_size), first, right, left, True)
    plane, result = lax.optimization_barrier((plane, result))
    back = exchange(result.reshape(outgoing.shape))
    return scatter_rows(table, back, 0, grad, all_planes(plane))


def second_core(grad, second_moment, left, right, table):
    block_size = left.shape[0]
    slots = lax.axis_size(DP)
    outgoing = gather_rows(table, grad, 1, slots, block_size)
    plane = plane_sums(grad, second_moment, block_size)
    parts = all_planes(plane)
    *parts[:3], outgoing = lax.optimization_barrier((*parts[:3], outgoing))
    rows_in = exchange(outgoing)
    own_table = jnp.transpose(table[1]).reshape(1, -1)
    first = fetch_columns(parts[-1], right, block_size // 2)
    result = own_block(
        rows_in.reshape(block_size, block_size), first, right, left, False, own_table, parts
    )
    back = exchange(result.reshape(outgoing.shape))
    return scatter_rows(table, back, 1, grad)


def per_device(grad, second_moment, left_root, right_root, owner_slot):
    table = jnp.transpose(owner_slot, (0, 2, 1))
    return lax.cond(
        lax.axis_index("mp") == 0,
        first_core,
        second_core,
        grad,
        second_moment,
        left_root[0, 0],
        right_root[0, 0],
        table,
    )


def solution(mesh):
    split = Mesh(mesh.devices.reshape(4, 8, 4, mesh.shape["mp"]), ("dp_0", "dp_1", "dp_2", "mp"))
    return jax.shard_map(
        per_device,
        mesh=split,
        in_specs=(
            P(None, DP, "mp"),
            P(None, DP, "mp"),
            P("mp", DP, None, None),
            P("mp", DP, None, None),
            P(),
        ),
        out_specs=P(None, DP, "mp"),
        check_vma=False,
    )
```

```python
import functools

import jax
import jax.numpy as jnp
from jax import lax
from jax.experimental import pallas as pl
from jax.experimental.pallas import tpu as pltpu
from jax.sharding import Mesh
from jax.sharding import PartitionSpec as P

DP = ("dp_0", "dp_1", "dp_2")


BETA_TWO = 0.99
ADAM_EPS = 1e-08
NORM_EPS = 1e-06
MIB = 1 << 20
VMEM = pl.BlockSpec(memory_space=pltpu.VMEM)
HBM = pl.BlockSpec(memory_space=pltpu.HBM)
SMEM = pl.BlockSpec(memory_space=pltpu.SMEM)


def in_hbm(value):
    return pltpu.with_memory_space_constraint(value, pltpu.HBM)


def gather_kernel(groups, half, table_hbm, grad_hbm, *refs):
    in_vmem = len(refs) > 6
    if in_vmem:
        right_hbm, out_ref, first_ref, table_ref, held_ref, table_sem, in_sem, out_sem = refs
    else:
        out_ref, table_ref, held_ref, table_sem, in_sem, out_sem = refs
    row_blocks = grad_hbm.shape[0]
    block_size = out_ref.shape[-1]
    col_blocks = grad_hbm.shape[2] // block_size
    group = row_blocks // groups

    def load(g):
        rows = pl.ds(g * group, group)
        return pltpu.make_async_copy(grad_hbm.at[rows], held_ref.at[rows], in_sem.at[g])

    table_load = pltpu.make_async_copy(table_hbm, table_ref, table_sem)
    table_load.start()
    for g in range(groups):
        load(g).start()
    if in_vmem:
        columns = right_hbm.at[:, pl.ds(0, first_ref.shape[1])]
        first_load = pltpu.make_async_copy(columns, first_ref, out_sem)
        first_load.start()
    table_load.wait()
    for g in range(groups):
        load(g).wait()

        def one_row(row, carry):
            for col in range(col_blocks):
                columns = pl.ds(col * block_size, block_size)
                slot = table_ref[half, col, row]
                if in_vmem:
                    out_ref[slot] = held_ref[row, :, columns]
                else:
                    pltpu.make_async_copy(held_ref.at[row, :, columns], out_ref.at[slot], out_sem).start()
            return carry

        lax.fori_loop(g * group, (g + 1) * group, one_row, 0)
    if in_vmem:
        first_load.wait()
    else:
        pltpu.make_async_copy(out_ref, out_ref, out_sem).wait()


def gather_rows(table, grad, half, slots, block_size, right=None):
    groups = 8
    shape = (slots, grad.shape[1], block_size)
    in_vmem = right is not None
    if in_vmem:
        rows = jax.ShapeDtypeStruct(shape, jnp.bfloat16)
        out_shape = (rows, jax.ShapeDtypeStruct((block_size, block_size // 2), jnp.bfloat16))
    else:
        out_shape = pltpu.HBM(shape, jnp.bfloat16)
    return pl.pallas_call(
        functools.partial(gather_kernel, groups, half),
        out_shape=out_shape,
        in_specs=[HBM, HBM] + [HBM] * in_vmem,
        out_specs=(VMEM, VMEM) if in_vmem else HBM,
        scratch_shapes=[
            pltpu.SMEM(table.shape, jnp.int32),
            pltpu.VMEM(grad.shape, jnp.bfloat16),
            pltpu.SemaphoreType.DMA,
            pltpu.SemaphoreType.DMA((groups,)),
            pltpu.SemaphoreType.DMA,
        ],
        compiler_params=pltpu.CompilerParams(vmem_limit_bytes=12 * MIB),
        name="gather_rows",
    )(in_hbm(table), in_hbm(grad), *([in_hbm(right)] if in_vmem else []))


def scatter_kernel(half, table_ref, back_ref, out_ref, held_ref, sem):
    row_blocks = out_ref.shape[0]
    block_size = back_ref.shape[-1]
    col_blocks = out_ref.shape[2] // block_size

    def one_row(row, carry):
        for col in range(col_blocks):
            columns = pl.ds(col * block_size, block_size)
            held_ref[row, :, columns] = back_ref[table_ref[half, col, row]]
        pltpu.make_async_copy(held_ref.at[row], out_ref.at[row], sem).start()
        return carry

    lax.fori_loop(0, row_blocks, one_row, 0)
    pltpu.make_async_copy(out_ref, out_ref, sem).wait()


def scaled_scatter_kernel(parts, half, table_ref, *refs):
    part_refs = refs[:parts]
    back_ref, out_ref, norm_ref, held_ref, sem = refs[parts:]
    row_blocks = out_ref.shape[0]
    block_size = back_ref.shape[-1]
    col_blocks = out_ref.shape[2] // block_size
    blocks = row_blocks * col_blocks
    totals = part_refs[0][...]
    for part_ref in part_refs[1:]:
        totals = totals + part_ref[...]
    norms = jnp.sqrt((totals[0:1] + NORM_EPS) / (totals[1:2] + NORM_EPS))
    norm_ref[...] = jnp.transpose(jnp.broadcast_to(norms, (blocks, blocks)))

    def one_row(row, carry):
        for col in range(col_blocks):
            slot = table_ref[half, col, row]
            norm = norm_ref[pl.ds(col * row_blocks + row, 1), :]
            norm = jnp.concatenate([norm] * (block_size // blocks), axis=1)
            rows = back_ref[slot].astype(jnp.float32) * norm
            held_ref[row, :, pl.ds(col * block_size, block_size)] = rows.astype(jnp.bfloat16)
        pltpu.make_async_copy(held_ref.at[row], out_ref.at[row], sem).start()
        return carry

    lax.fori_loop(0, row_blocks, one_row, 0)
    pltpu.make_async_copy(out_ref, out_ref, sem).wait()


def scatter_rows(table, back, half, like, parts=None):
    out_shape = pltpu.HBM(like.shape, jnp.bfloat16)
    params = pltpu.CompilerParams(vmem_limit_bytes=8 * MIB)
    if parts is None:
        return pl.pallas_call(
            functools.partial(scatter_kernel, half),
            out_shape=out_shape,
            in_specs=[SMEM, VMEM],
            out_specs=HBM,
            scratch_shapes=[pltpu.VMEM(like.shape, jnp.bfloat16), pltpu.SemaphoreType.DMA],
            compiler_params=params,
            name="scatter_rows",
        )(table, back)
    blocks = parts[0].shape[1]
    return pl.pallas_call(
        functools.partial(scaled_scatter_kernel, len(parts), half),
        out_shape=out_shape,
        in_specs=[SMEM] + [VMEM] * (len(parts) + 1),
        out_specs=HBM,
        scratch_shapes=[
            pltpu.VMEM((blocks, blocks), jnp.float32),
            pltpu.VMEM(like.shape, jnp.bfloat16),
            pltpu.SemaphoreType.DMA,
        ],
        compiler_params=params,
        name="scaled_scatter_rows",
    )(table, *parts, back)


def fetch_kernel(after_ref, right_hbm, out_ref, sem):
    columns = right_hbm.at[:, pl.ds(0, out_ref.shape[1])]
    copy = pltpu.make_async_copy(columns, out_ref, sem)
    copy.start()
    copy.wait()


def fetch_columns(after, right, columns):
    return pl.pallas_call(
        fetch_kernel,
        out_shape=jax.ShapeDtypeStruct((right.shape[0], columns), jnp.bfloat16),
        in_specs=[VMEM, HBM],
        out_specs=VMEM,
        scratch_shapes=[pltpu.SemaphoreType.DMA],
        compiler_params=pltpu.CompilerParams(vmem_limit_bytes=8 * MIB),
        name="fetch_columns",
    )(after, in_hbm(right))


def owners(table_ref, half):
    table = table_ref[half]
    return jnp.concatenate([table[col : col + 1] for col in range(table.shape[0])], axis=1)


def block_kernel(half, table_ref, *refs):
    parts = len(refs) - 10
    part_refs = refs[:parts]
    rows_ref, first_ref, right_hbm, left_hbm, out_ref, right_ref, left_ref, mixed_ref, shaped_ref, sem = refs[parts:]
    block_size = right_hbm.shape[0]
    tile = first_ref.shape[1]
    loads = start_loads(right_hbm, left_hbm, right_ref, left_ref, tile, sem)
    totals = part_refs[0][...]
    for part_ref in part_refs[1:]:
        totals = totals + part_ref[...]
    adam_sq = jnp.sum(jnp.where(owners(table_ref, half) == lax.axis_index(DP), totals, 0.0))
    mix(rows_ref, first_ref, right_ref, mixed_ref, tile, loads)

    def shape(j, squares):
        cols = pl.ds(pl.multiple_of(j * tile, tile), tile)
        shaped = jnp.dot(left_ref[...], mixed_ref[:, cols], preferred_element_type=jnp.float32)
        shaped_ref[:, cols] = shaped
        return squares + jnp.sum((shaped * shaped).reshape(block_size // 8, 8, tile), axis=0)

    squares = lax.fori_loop(0, block_size // tile, shape, jnp.zeros((8, tile), jnp.float32))
    shaped_sq = jnp.full((8, 128), jnp.sum(squares), jnp.float32)
    scale = jnp.sqrt((adam_sq + NORM_EPS) / (shaped_sq + NORM_EPS))[0:1, 0:1]
    band = block_size // 4

    def finish(i, carry):
        rows = pl.ds(pl.multiple_of(i * band, band), band)
        out_ref[rows, :] = (shaped_ref[rows, :] * scale).astype(jnp.bfloat16)
        return carry

    lax.fori_loop(0, 4, finish, 0)


def raw_block_kernel(
    half, table_ref, rows_ref, first_ref, right_hbm, left_hbm, out_hbm, square_ref, right_ref, left_ref, mixed_ref, held_ref, sem
):
    block_size = right_hbm.shape[0]
    tile = first_ref.shape[1]
    steps = block_size // tile
    loads = start_loads(right_hbm, left_hbm, right_ref, left_ref, tile, sem)
    mix(rows_ref, first_ref, right_ref, mixed_ref, tile, loads)

    def store(j):
        cols = pl.ds(pl.multiple_of(j * tile, tile), tile)
        return pltpu.make_async_copy(held_ref.at[:, cols], out_hbm.at[:, cols], sem.at[j])

    def shape(j, squares):
        cols = pl.ds(pl.multiple_of(j * tile, tile), tile)
        shaped = jnp.dot(left_ref[...], mixed_ref[:, cols], preferred_element_type=jnp.float32)
        held_ref[:, cols] = shaped.astype(jnp.bfloat16)
        store(j).start()
        return squares + jnp.sum((shaped * shaped).reshape(block_size // 8, 8, tile), axis=0)

    squares = lax.fori_loop(0, steps, shape, jnp.zeros((8, tile), jnp.float32))
    square_ref[...] = jnp.where(owners(table_ref, half) == lax.axis_index(DP), jnp.sum(squares), 0.0)
    for j in range(steps):
        store(j).wait()


def start_loads(right_hbm, left_hbm, right_ref, left_ref, tile, sem):
    rest = pl.ds(tile, right_hbm.shape[1] - tile)
    right_load = pltpu.make_async_copy(right_hbm.at[:, rest], right_ref.at[:, rest], sem.at[0])
    left_load = pltpu.make_async_copy(left_hbm, left_ref, sem.at[1])
    right_load.start()
    left_load.start()
    return right_load, left_load


def mix(rows_ref, first_ref, right_ref, mixed_ref, tile, loads):
    for start in range(0, mixed_ref.shape[1], tile):
        cols = pl.ds(start, tile)
        if start == tile:
            loads[0].wait()
        columns = right_ref[:, cols] if start > 0 else first_ref[...]
        mixed = jnp.dot(rows_ref[...], columns, preferred_element_type=jnp.float32)
        mixed_ref[:, cols] = mixed.astype(jnp.bfloat16)
    loads[1].wait()


def own_block(rows_in, first, right, left, table, half, parts=()):
    block_size = right.shape[0]
    shape = (block_size, block_size)
    square = pltpu.VMEM(shape, jnp.bfloat16)
    finished = len(parts) > 0
    if finished:
        kernel, held = block_kernel, pltpu.VMEM(shape, jnp.float32)
        out_shape = jax.ShapeDtypeStruct(shape, jnp.bfloat16)
    else:
        kernel, held = raw_block_kernel, square
        out_shape = (pltpu.HBM(shape, jnp.bfloat16), jax.ShapeDtypeStruct((1, table[0].size), jnp.float32))
    return pl.pallas_call(
        functools.partial(kernel, half),
        out_shape=out_shape,
        in_specs=[VMEM] * (len(parts) + 3) + [HBM] * 2,
        out_specs=VMEM if finished else (HBM, VMEM),
        scratch_shapes=[square, square, square, held, pltpu.SemaphoreType.DMA((2,))],
        compiler_params=pltpu.CompilerParams(vmem_limit_bytes=24 * MIB),
        name="own_block" if finished else "raw_block",
        cost_estimate=pl.CostEstimate(
            flops=4 * block_size**3, bytes_accessed=8 * block_size**2, transcendentals=0
        ),
    )(table, *parts, rows_in, first, in_hbm(right), in_hbm(left))


def exchange(value):
    return lax.all_to_all(value, DP, split_axis=0, concat_axis=0, tiled=True)


def adam_sums(grad, second_moment, block_size):
    row_blocks, block_rows, half_cols = grad.shape
    col_blocks = half_cols // block_size
    widened = grad.astype(jnp.float32)
    moment_new = BETA_TWO * second_moment + (1.0 - BETA_TWO) * widened * widened
    direction = widened / (jnp.sqrt(moment_new) + ADAM_EPS)
    sums = jnp.sum(
        (direction * direction).reshape(row_blocks, block_rows, col_blocks, block_size), axis=(1, 3)
    )
    return jnp.transpose(sums).reshape(1, row_blocks * col_blocks)


def plane_sums(value):
    return lax.psum(lax.psum(value, "dp_0"), "dp_2")


def all_planes(plane):
    depth = lax.axis_size("dp_1")
    parts = [plane]
    for step in range(1, depth):
        ring = [(i, (i + step) % depth) for i in range(depth)]
        parts.append(lax.ppermute(plane, "dp_1", ring))
    return parts


def first_core(grad, second_moment, left, right, table):
    block_size = left.shape[0]
    slots = lax.axis_size(DP)
    outgoing, first = gather_rows(table, grad, 0, slots, block_size, right)
    rows_in = exchange(outgoing)
    result, square = own_block(
        rows_in.reshape(block_size, block_size), first, right, left, table, 0
    )
    second_moment, result = lax.optimization_barrier((second_moment, result))
    back = exchange(result.reshape(outgoing.shape))
    sums = jnp.concatenate([adam_sums(grad, second_moment, block_size), square], axis=0)
    return scatter_rows(table, back, 0, grad, all_planes(plane_sums(sums)))


def second_core(grad, second_moment, left, right, table):
    block_size = left.shape[0]
    outgoing = gather_rows(table, grad, 1, lax.axis_size(DP), block_size)
    parts = all_planes(plane_sums(adam_sums(grad, second_moment, block_size)))
    *parts[:3], outgoing = lax.optimization_barrier((*parts[:3], outgoing))
    rows_in = exchange(outgoing)
    first = fetch_columns(parts[-1], right, block_size // 2)
    result = own_block(
        rows_in.reshape(block_size, block_size), first, right, left, table, 1, parts
    )
    back = exchange(result.reshape(outgoing.shape))
    return scatter_rows(table, back, 1, grad)


def per_device(grad, second_moment, left_root, right_root, owner_slot):
    table = jnp.transpose(owner_slot, (0, 2, 1))
    return lax.cond(
        lax.axis_index("mp") == 0,
        first_core,
        second_core,
        grad,
        second_moment,
        left_root[0, 0],
        right_root[0, 0],
        table,
    )


def solution(mesh):
    split = Mesh(mesh.devices.reshape(4, 8, 4, mesh.shape["mp"]), ("dp_0", "dp_1", "dp_2", "mp"))
    return jax.shard_map(
        per_device,
        mesh=split,
        in_specs=(
            P(None, DP, "mp"),
            P(None, DP, "mp"),
            P("mp", DP, None, None),
            P("mp", DP, None, None),
            P(),
        ),
        out_specs=P(None, DP, "mp"),
        check_vma=False,
    )
```

```python
import functools

import jax
import jax.numpy as jnp
from jax import lax
from jax.experimental import pallas as pl
from jax.experimental.pallas import tpu as pltpu
from jax.sharding import Mesh
from jax.sharding import PartitionSpec as P

DP = ("dp_0", "dp_1", "dp_2")


BETA_TWO = 0.99
ADAM_EPS = 1e-08
NORM_EPS = 1e-06
MIB = 1 << 20
VMEM = pl.BlockSpec(memory_space=pltpu.VMEM)
HBM = pl.BlockSpec(memory_space=pltpu.HBM)
SMEM = pl.BlockSpec(memory_space=pltpu.SMEM)


def in_hbm(value):
    return pltpu.with_memory_space_constraint(value, pltpu.HBM)


def gather_kernel(groups, half, table_hbm, grad_hbm, *refs):
    in_vmem = len(refs) > 6
    if in_vmem:
        right_hbm, out_ref, first_ref, table_ref, held_ref, table_sem, in_sem, out_sem = refs
    else:
        out_ref, table_ref, held_ref, table_sem, in_sem, out_sem = refs
    row_blocks = grad_hbm.shape[0]
    block_size = out_ref.shape[-1]
    col_blocks = grad_hbm.shape[2] // block_size
    group = row_blocks // groups

    def load(g):
        rows = pl.ds(g * group, group)
        return pltpu.make_async_copy(grad_hbm.at[rows], held_ref.at[rows], in_sem.at[g])

    table_load = pltpu.make_async_copy(table_hbm, table_ref, table_sem)
    table_load.start()
    for g in range(groups):
        load(g).start()
    if in_vmem:
        columns = right_hbm.at[:, pl.ds(0, first_ref.shape[1])]
        first_load = pltpu.make_async_copy(columns, first_ref, out_sem)
        first_load.start()
    table_load.wait()
    for g in range(groups):
        load(g).wait()

        def one_row(row, carry):
            for col in range(col_blocks):
                columns = pl.ds(col * block_size, block_size)
                slot = table_ref[half, col, row]
                if in_vmem:
                    out_ref[slot] = held_ref[row, :, columns]
                else:
                    pltpu.make_async_copy(held_ref.at[row, :, columns], out_ref.at[slot], out_sem).start()
            return carry

        lax.fori_loop(g * group, (g + 1) * group, one_row, 0)
    if in_vmem:
        first_load.wait()
    else:
        pltpu.make_async_copy(out_ref, out_ref, out_sem).wait()


def gather_rows(table, grad, half, slots, block_size, right=None):
    groups = 8
    shape = (slots, grad.shape[1], block_size)
    in_vmem = right is not None
    if in_vmem:
        rows = jax.ShapeDtypeStruct(shape, jnp.bfloat16)
        out_shape = (rows, jax.ShapeDtypeStruct((block_size, block_size // 2), jnp.bfloat16))
    else:
        out_shape = pltpu.HBM(shape, jnp.bfloat16)
    return pl.pallas_call(
        functools.partial(gather_kernel, groups, half),
        out_shape=out_shape,
        in_specs=[HBM, HBM] + [HBM] * in_vmem,
        out_specs=(VMEM, VMEM) if in_vmem else HBM,
        scratch_shapes=[
            pltpu.SMEM(table.shape, jnp.int32),
            pltpu.VMEM(grad.shape, jnp.bfloat16),
            pltpu.SemaphoreType.DMA,
            pltpu.SemaphoreType.DMA((groups,)),
            pltpu.SemaphoreType.DMA,
        ],
        compiler_params=pltpu.CompilerParams(vmem_limit_bytes=12 * MIB),
        name="gather_rows",
    )(in_hbm(table), in_hbm(grad), *([in_hbm(right)] if in_vmem else []))


def scatter_kernel(half, table_ref, back_ref, out_ref, held_ref, sem):
    row_blocks = out_ref.shape[0]
    block_size = back_ref.shape[-1]
    col_blocks = out_ref.shape[2] // block_size

    def one_row(row, carry):
        for col in range(col_blocks):
            columns = pl.ds(col * block_size, block_size)
            held_ref[row, :, columns] = back_ref[table_ref[half, col, row]]
        pltpu.make_async_copy(held_ref.at[row], out_ref.at[row], sem).start()
        return carry

    lax.fori_loop(0, row_blocks, one_row, 0)
    pltpu.make_async_copy(out_ref, out_ref, sem).wait()


def scaled_scatter_kernel(parts, half, table_ref, *refs):
    part_refs = refs[:parts]
    back_ref, out_ref, norm_ref, held_ref, sem = refs[parts:]
    row_blocks = out_ref.shape[0]
    block_size = back_ref.shape[-1]
    col_blocks = out_ref.shape[2] // block_size
    blocks = row_blocks * col_blocks
    totals = part_refs[0][...]
    for part_ref in part_refs[1:]:
        totals = totals + part_ref[...]
    norms = jnp.sqrt((totals[0:1] + NORM_EPS) / (totals[1:2] + NORM_EPS))
    norm_ref[...] = jnp.transpose(jnp.broadcast_to(norms, (blocks, blocks)))

    def one_row(row, carry):
        for col in range(col_blocks):
            slot = table_ref[half, col, row]
            norm = norm_ref[pl.ds(col * row_blocks + row, 1), :]
            norm = jnp.concatenate([norm] * (block_size // blocks), axis=1)
            rows = back_ref[slot].astype(jnp.float32) * norm
            held_ref[row, :, pl.ds(col * block_size, block_size)] = rows.astype(jnp.bfloat16)
        pltpu.make_async_copy(held_ref.at[row], out_ref.at[row], sem).start()
        return carry

    lax.fori_loop(0, row_blocks, one_row, 0)
    pltpu.make_async_copy(out_ref, out_ref, sem).wait()


def scatter_rows(table, back, half, like, parts=None):
    out_shape = pltpu.HBM(like.shape, jnp.bfloat16)
    params = pltpu.CompilerParams(vmem_limit_bytes=8 * MIB)
    if parts is None:
        return pl.pallas_call(
            functools.partial(scatter_kernel, half),
            out_shape=out_shape,
            in_specs=[SMEM, VMEM],
            out_specs=HBM,
            scratch_shapes=[pltpu.VMEM(like.shape, jnp.bfloat16), pltpu.SemaphoreType.DMA],
            compiler_params=params,
            name="scatter_rows",
        )(table, back)
    blocks = parts[0].shape[1]
    return pl.pallas_call(
        functools.partial(scaled_scatter_kernel, len(parts), half),
        out_shape=out_shape,
        in_specs=[SMEM] + [VMEM] * (len(parts) + 1),
        out_specs=HBM,
        scratch_shapes=[
            pltpu.VMEM((blocks, blocks), jnp.float32),
            pltpu.VMEM(like.shape, jnp.bfloat16),
            pltpu.SemaphoreType.DMA,
        ],
        compiler_params=params,
        name="scaled_scatter_rows",
    )(table, *parts, back)


def fetch_kernel(after_ref, right_hbm, out_ref, sem):
    columns = right_hbm.at[:, pl.ds(0, out_ref.shape[1])]
    copy = pltpu.make_async_copy(columns, out_ref, sem)
    copy.start()
    copy.wait()


def fetch_columns(after, right, columns):
    return pl.pallas_call(
        fetch_kernel,
        out_shape=jax.ShapeDtypeStruct((right.shape[0], columns), jnp.bfloat16),
        in_specs=[VMEM, HBM],
        out_specs=VMEM,
        scratch_shapes=[pltpu.SemaphoreType.DMA],
        compiler_params=pltpu.CompilerParams(vmem_limit_bytes=8 * MIB),
        name="fetch_columns",
    )(after, in_hbm(right))


def owners(table_ref, half):
    table = table_ref[half]
    return jnp.concatenate([table[col : col + 1] for col in range(table.shape[0])], axis=1)


def block_kernel(half, table_ref, *refs):
    parts = len(refs) - 10
    part_refs = refs[:parts]
    rows_ref, first_ref, right_hbm, left_hbm, out_ref, right_ref, left_ref, mixed_ref, shaped_ref, sem = refs[parts:]
    block_size = right_hbm.shape[0]
    tile = first_ref.shape[1]
    loads = start_loads(right_hbm, left_hbm, right_ref, left_ref, tile, sem)
    totals = part_refs[0][...]
    for part_ref in part_refs[1:]:
        totals = totals + part_ref[...]
    adam_sq = jnp.sum(jnp.where(owners(table_ref, half) == lax.axis_index(DP), totals, 0.0))
    mix(rows_ref, first_ref, right_ref, mixed_ref, tile, loads)

    def shape(j, squares):
        cols = pl.ds(pl.multiple_of(j * tile, tile), tile)
        shaped = jnp.dot(left_ref[...], mixed_ref[:, cols], preferred_element_type=jnp.float32)
        shaped_ref[:, cols] = shaped
        return squares + jnp.sum((shaped * shaped).reshape(block_size // 8, 8, tile), axis=0)

    squares = lax.fori_loop(0, block_size // tile, shape, jnp.zeros((8, tile), jnp.float32))
    shaped_sq = jnp.full((8, 128), jnp.sum(squares), jnp.float32)
    scale = jnp.sqrt((adam_sq + NORM_EPS) / (shaped_sq + NORM_EPS))[0:1, 0:1]
    band = block_size // 4

    def finish(i, carry):
        rows = pl.ds(pl.multiple_of(i * band, band), band)
        out_ref[rows, :] = (shaped_ref[rows, :] * scale).astype(jnp.bfloat16)
        return carry

    lax.fori_loop(0, 4, finish, 0)


def raw_block_kernel(
    half, table_ref, rows_ref, first_ref, right_hbm, left_hbm, out_hbm, square_ref, right_ref, left_ref, mixed_ref, held_ref, sem
):
    block_size = right_hbm.shape[0]
    tile = first_ref.shape[1]
    steps = block_size // tile
    loads = start_loads(right_hbm, left_hbm, right_ref, left_ref, tile, sem)
    mix(rows_ref, first_ref, right_ref, mixed_ref, tile, loads)

    def store(j):
        cols = pl.ds(pl.multiple_of(j * tile, tile), tile)
        return pltpu.make_async_copy(held_ref.at[:, cols], out_hbm.at[:, cols], sem.at[j])

    def shape(j, squares):
        cols = pl.ds(pl.multiple_of(j * tile, tile), tile)
        shaped = jnp.dot(left_ref[...], mixed_ref[:, cols], preferred_element_type=jnp.float32)
        held_ref[:, cols] = shaped.astype(jnp.bfloat16)
        store(j).start()
        return squares + jnp.sum((shaped * shaped).reshape(block_size // 8, 8, tile), axis=0)

    squares = lax.fori_loop(0, steps, shape, jnp.zeros((8, tile), jnp.float32))
    square_ref[...] = jnp.where(owners(table_ref, half) == lax.axis_index(DP), jnp.sum(squares), 0.0)
    for j in range(steps):
        store(j).wait()


def start_loads(right_hbm, left_hbm, right_ref, left_ref, tile, sem):
    rest = pl.ds(tile, right_hbm.shape[1] - tile)
    right_load = pltpu.make_async_copy(right_hbm.at[:, rest], right_ref.at[:, rest], sem.at[0])
    left_load = pltpu.make_async_copy(left_hbm, left_ref, sem.at[1])
    right_load.start()
    left_load.start()
    return right_load, left_load


def mix(rows_ref, first_ref, right_ref, mixed_ref, tile, loads):
    for start in range(0, mixed_ref.shape[1], tile):
        cols = pl.ds(start, tile)
        if start == tile:
            loads[0].wait()
        columns = right_ref[:, cols] if start > 0 else first_ref[...]
        mixed = jnp.dot(rows_ref[...], columns, preferred_element_type=jnp.float32)
        mixed_ref[:, cols] = mixed.astype(jnp.bfloat16)
    loads[1].wait()


def own_block(rows_in, first, right, left, table, half, parts=()):
    block_size = right.shape[0]
    shape = (block_size, block_size)
    square = pltpu.VMEM(shape, jnp.bfloat16)
    finished = len(parts) > 0
    if finished:
        kernel, held = block_kernel, pltpu.VMEM(shape, jnp.float32)
        out_shape = jax.ShapeDtypeStruct(shape, jnp.bfloat16)
    else:
        kernel, held = raw_block_kernel, square
        out_shape = (pltpu.HBM(shape, jnp.bfloat16), jax.ShapeDtypeStruct((1, table[0].size), jnp.float32))
    return pl.pallas_call(
        functools.partial(kernel, half),
        out_shape=out_shape,
        in_specs=[VMEM] * (len(parts) + 3) + [HBM] * 2,
        out_specs=VMEM if finished else (HBM, VMEM),
        scratch_shapes=[square, square, square, held, pltpu.SemaphoreType.DMA((2,))],
        compiler_params=pltpu.CompilerParams(vmem_limit_bytes=24 * MIB),
        name="own_block" if finished else "raw_block",
        cost_estimate=pl.CostEstimate(
            flops=4 * block_size**3, bytes_accessed=8 * block_size**2, transcendentals=0
        ),
    )(table, *parts, rows_in, first, in_hbm(right), in_hbm(left))


def exchange(value):
    return lax.all_to_all(value, DP, split_axis=0, concat_axis=0, tiled=True)


def adam_sums(grad, second_moment, block_size):
    row_blocks, block_rows, half_cols = grad.shape
    col_blocks = half_cols // block_size
    widened = grad.astype(jnp.float32)
    square = widened * widened
    moment_new = BETA_TWO * second_moment + (1.0 - BETA_TWO) * square
    root = moment_new * lax.rsqrt(moment_new)
    ratio = square / (moment_new + ADAM_EPS * (2.0 * root + ADAM_EPS))
    sums = jnp.sum(ratio.reshape(row_blocks, block_rows, col_blocks, block_size), axis=(1, 3))
    return jnp.transpose(sums).reshape(1, row_blocks * col_blocks)


def plane_sums(value):
    return lax.psum(lax.psum(value, "dp_0"), "dp_2")


def all_planes(plane):
    depth = lax.axis_size("dp_1")
    parts = [plane]
    for step in range(1, depth):
        ring = [(i, (i + step) % depth) for i in range(depth)]
        parts.append(lax.ppermute(plane, "dp_1", ring))
    return parts


def first_core(grad, second_moment, left, right, table):
    block_size = left.shape[0]
    slots = lax.axis_size(DP)
    outgoing, first = gather_rows(table, grad, 0, slots, block_size, right)
    rows_in = exchange(outgoing)
    result, square = own_block(
        rows_in.reshape(block_size, block_size), first, right, left, table, 0
    )
    second_moment, result = lax.optimization_barrier((second_moment, result))
    back = exchange(result.reshape(outgoing.shape))
    sums = jnp.concatenate([adam_sums(grad, second_moment, block_size), square], axis=0)
    return scatter_rows(table, back, 0, grad, all_planes(plane_sums(sums)))


def second_core(grad, second_moment, left, right, table):
    block_size = left.shape[0]
    outgoing = gather_rows(table, grad, 1, lax.axis_size(DP), block_size)
    parts = all_planes(plane_sums(adam_sums(grad, second_moment, block_size)))
    *parts[:3], outgoing = lax.optimization_barrier((*parts[:3], outgoing))
    rows_in = exchange(outgoing)
    first = fetch_columns(parts[-1], right, block_size // 2)
    result = own_block(
        rows_in.reshape(block_size, block_size), first, right, left, table, 1, parts
    )
    back = exchange(result.reshape(outgoing.shape))
    return scatter_rows(table, back, 1, grad)


def per_device(grad, second_moment, left_root, right_root, owner_slot):
    table = jnp.transpose(owner_slot, (0, 2, 1))
    return lax.cond(
        lax.axis_index("mp") == 0,
        first_core,
        second_core,
        grad,
        second_moment,
        left_root[0, 0],
        right_root[0, 0],
        table,
    )


def solution(mesh):
    split = Mesh(mesh.devices.reshape(4, 8, 4, mesh.shape["mp"]), ("dp_0", "dp_1", "dp_2", "mp"))
    return jax.shard_map(
        per_device,
        mesh=split,
        in_specs=(
            P(None, DP, "mp"),
            P(None, DP, "mp"),
            P("mp", DP, None, None),
            P("mp", DP, None, None),
            P(),
        ),
        out_specs=P(None, DP, "mp"),
        check_vma=False,
    )
```

```python
import functools

import jax
import jax.numpy as jnp
from jax import lax
from jax.experimental import pallas as pl
from jax.experimental.pallas import tpu as pltpu
from jax.sharding import Mesh
from jax.sharding import PartitionSpec as P

DP = ("dp_0", "dp_1", "dp_2")


BETA_TWO = 0.99
ADAM_EPS = 1e-08
NORM_EPS = 1e-06
MIB = 1 << 20
VMEM = pl.BlockSpec(memory_space=pltpu.VMEM)
HBM = pl.BlockSpec(memory_space=pltpu.HBM)
SMEM = pl.BlockSpec(memory_space=pltpu.SMEM)


def in_hbm(value):
    return pltpu.with_memory_space_constraint(value, pltpu.HBM)


def gather_kernel(groups, half, table_hbm, grad_hbm, *refs):
    in_vmem = len(refs) > 6
    if in_vmem:
        right_hbm, out_ref, first_ref, table_ref, held_ref, table_sem, in_sem, out_sem = refs
    else:
        out_ref, table_ref, held_ref, table_sem, in_sem, out_sem = refs
    row_blocks = grad_hbm.shape[0]
    block_size = out_ref.shape[-1]
    col_blocks = grad_hbm.shape[2] // block_size
    group = row_blocks // groups

    def load(g):
        rows = pl.ds(g * group, group)
        return pltpu.make_async_copy(grad_hbm.at[rows], held_ref.at[rows], in_sem.at[g])

    table_load = pltpu.make_async_copy(table_hbm, table_ref, table_sem)
    table_load.start()
    for g in range(groups):
        load(g).start()
    if in_vmem:
        columns = right_hbm.at[:, pl.ds(0, first_ref.shape[1])]
        first_load = pltpu.make_async_copy(columns, first_ref, out_sem)
        first_load.start()
    table_load.wait()
    for g in range(groups):
        load(g).wait()

        def one_row(row, carry):
            for col in range(col_blocks):
                columns = pl.ds(col * block_size, block_size)
                slot = table_ref[half, col, row]
                if in_vmem:
                    out_ref[slot] = held_ref[row, :, columns]
                else:
                    pltpu.make_async_copy(held_ref.at[row, :, columns], out_ref.at[slot], out_sem).start()
            return carry

        lax.fori_loop(g * group, (g + 1) * group, one_row, 0)
    if in_vmem:
        first_load.wait()
    else:
        pltpu.make_async_copy(out_ref, out_ref, out_sem).wait()


def gather_rows(table, grad, half, slots, block_size, right=None):
    groups = 8
    shape = (slots, grad.shape[1], block_size)
    in_vmem = right is not None
    if in_vmem:
        rows = jax.ShapeDtypeStruct(shape, jnp.bfloat16)
        out_shape = (rows, jax.ShapeDtypeStruct((block_size, block_size // 2), jnp.bfloat16))
    else:
        out_shape = pltpu.HBM(shape, jnp.bfloat16)
    return pl.pallas_call(
        functools.partial(gather_kernel, groups, half),
        out_shape=out_shape,
        in_specs=[HBM, HBM] + [HBM] * in_vmem,
        out_specs=(VMEM, VMEM) if in_vmem else HBM,
        scratch_shapes=[
            pltpu.SMEM(table.shape, jnp.int32),
            pltpu.VMEM(grad.shape, jnp.bfloat16),
            pltpu.SemaphoreType.DMA,
            pltpu.SemaphoreType.DMA((groups,)),
            pltpu.SemaphoreType.DMA,
        ],
        compiler_params=pltpu.CompilerParams(vmem_limit_bytes=12 * MIB),
        name="gather_rows",
    )(in_hbm(table), in_hbm(grad), *([in_hbm(right)] if in_vmem else []))


def scatter_kernel(half, table_ref, back_ref, out_ref, held_ref, sem):
    row_blocks = out_ref.shape[0]
    block_size = back_ref.shape[-1]
    col_blocks = out_ref.shape[2] // block_size

    def one_row(row, carry):
        for col in range(col_blocks):
            columns = pl.ds(col * block_size, block_size)
            held_ref[row, :, columns] = back_ref[table_ref[half, col, row]]
        pltpu.make_async_copy(held_ref.at[row], out_ref.at[row], sem).start()
        return carry

    lax.fori_loop(0, row_blocks, one_row, 0)
    pltpu.make_async_copy(out_ref, out_ref, sem).wait()


def scaled_scatter_kernel(parts, half, table_ref, *refs):
    part_refs = refs[:parts]
    back_ref, out_ref, norm_ref, held_ref, sem = refs[parts:]
    row_blocks = out_ref.shape[0]
    block_size = back_ref.shape[-1]
    col_blocks = out_ref.shape[2] // block_size
    blocks = row_blocks * col_blocks
    totals = part_refs[0][...]
    for part_ref in part_refs[1:]:
        totals = totals + part_ref[...]
    norms = jnp.sqrt((totals[0:1] + NORM_EPS) / (totals[1:2] + NORM_EPS))
    norm_ref[...] = jnp.transpose(jnp.broadcast_to(norms, (blocks, blocks)))

    def one_row(row, carry):
        for col in range(col_blocks):
            slot = table_ref[half, col, row]
            norm = norm_ref[pl.ds(col * row_blocks + row, 1), :]
            norm = jnp.concatenate([norm] * (block_size // blocks), axis=1)
            rows = back_ref[slot].astype(jnp.float32) * norm
            held_ref[row, :, pl.ds(col * block_size, block_size)] = rows.astype(jnp.bfloat16)
        pltpu.make_async_copy(held_ref.at[row], out_ref.at[row], sem).start()
        return carry

    lax.fori_loop(0, row_blocks, one_row, 0)
    pltpu.make_async_copy(out_ref, out_ref, sem).wait()


def scatter_rows(table, back, half, like, parts=None):
    out_shape = pltpu.HBM(like.shape, jnp.bfloat16)
    params = pltpu.CompilerParams(vmem_limit_bytes=8 * MIB)
    if parts is None:
        return pl.pallas_call(
            functools.partial(scatter_kernel, half),
            out_shape=out_shape,
            in_specs=[SMEM, VMEM],
            out_specs=HBM,
            scratch_shapes=[pltpu.VMEM(like.shape, jnp.bfloat16), pltpu.SemaphoreType.DMA],
            compiler_params=params,
            name="scatter_rows",
        )(table, back)
    blocks = parts[0].shape[1]
    return pl.pallas_call(
        functools.partial(scaled_scatter_kernel, len(parts), half),
        out_shape=out_shape,
        in_specs=[SMEM] + [VMEM] * (len(parts) + 1),
        out_specs=HBM,
        scratch_shapes=[
            pltpu.VMEM((blocks, blocks), jnp.float32),
            pltpu.VMEM(like.shape, jnp.bfloat16),
            pltpu.SemaphoreType.DMA,
        ],
        compiler_params=params,
        name="scaled_scatter_rows",
    )(table, *parts, back)


def fetch_kernel(after_ref, right_hbm, out_ref, sem):
    columns = right_hbm.at[:, pl.ds(0, out_ref.shape[1])]
    copy = pltpu.make_async_copy(columns, out_ref, sem)
    copy.start()
    copy.wait()


def fetch_columns(after, right, columns):
    return pl.pallas_call(
        fetch_kernel,
        out_shape=jax.ShapeDtypeStruct((right.shape[0], columns), jnp.bfloat16),
        in_specs=[VMEM, HBM],
        out_specs=VMEM,
        scratch_shapes=[pltpu.SemaphoreType.DMA],
        compiler_params=pltpu.CompilerParams(vmem_limit_bytes=8 * MIB),
        name="fetch_columns",
    )(after, in_hbm(right))


def owners(table_ref, half):
    table = table_ref[half]
    return jnp.concatenate([table[col : col + 1] for col in range(table.shape[0])], axis=1)


def block_kernel(half, table_ref, *refs):
    parts = len(refs) - 10
    part_refs = refs[:parts]
    rows_ref, first_ref, right_hbm, left_hbm, out_ref, right_ref, left_ref, mixed_ref, shaped_ref, sem = refs[parts:]
    block_size = right_hbm.shape[0]
    tile = first_ref.shape[1]
    loads = start_loads(right_hbm, left_hbm, right_ref, left_ref, tile, sem)
    totals = part_refs[0][...]
    for part_ref in part_refs[1:]:
        totals = totals + part_ref[...]
    adam_sq = jnp.sum(jnp.where(owners(table_ref, half) == lax.axis_index(DP), totals, 0.0))
    mix(rows_ref, first_ref, right_ref, mixed_ref, tile, loads)

    def shape(j, squares):
        cols = pl.ds(pl.multiple_of(j * tile, tile), tile)
        shaped = jnp.dot(left_ref[...], mixed_ref[:, cols], preferred_element_type=jnp.float32)
        shaped_ref[:, cols] = shaped
        return squares + jnp.sum((shaped * shaped).reshape(block_size // 8, 8, tile), axis=0)

    squares = lax.fori_loop(0, block_size // tile, shape, jnp.zeros((8, tile), jnp.float32))
    shaped_sq = jnp.full((8, 128), jnp.sum(squares), jnp.float32)
    scale = jnp.sqrt((adam_sq + NORM_EPS) / (shaped_sq + NORM_EPS))[0:1, 0:1]
    band = block_size // 4

    def finish(i, carry):
        rows = pl.ds(pl.multiple_of(i * band, band), band)
        out_ref[rows, :] = (shaped_ref[rows, :] * scale).astype(jnp.bfloat16)
        return carry

    lax.fori_loop(0, 4, finish, 0)


def raw_block_kernel(
    half, table_ref, rows_ref, first_ref, right_hbm, left_hbm, out_hbm, square_ref, right_ref, left_ref, mixed_ref, held_ref, sem
):
    block_size = right_hbm.shape[0]
    tile = first_ref.shape[1]
    steps = block_size // tile
    loads = start_loads(right_hbm, left_hbm, right_ref, left_ref, tile, sem)
    mix(rows_ref, first_ref, right_ref, mixed_ref, tile, loads)

    def store(j):
        cols = pl.ds(pl.multiple_of(j * tile, tile), tile)
        return pltpu.make_async_copy(held_ref.at[:, cols], out_hbm.at[:, cols], sem.at[j])

    def shape(j, squares):
        cols = pl.ds(pl.multiple_of(j * tile, tile), tile)
        shaped = jnp.dot(left_ref[...], mixed_ref[:, cols], preferred_element_type=jnp.float32)
        held_ref[:, cols] = shaped.astype(jnp.bfloat16)
        store(j).start()
        return squares + jnp.sum((shaped * shaped).reshape(block_size // 8, 8, tile), axis=0)

    squares = lax.fori_loop(0, steps, shape, jnp.zeros((8, tile), jnp.float32))
    square_ref[...] = jnp.where(owners(table_ref, half) == lax.axis_index(DP), jnp.sum(squares), 0.0)
    for j in range(steps):
        store(j).wait()


def start_loads(right_hbm, left_hbm, right_ref, left_ref, tile, sem):
    rest = pl.ds(tile, right_hbm.shape[1] - tile)
    right_load = pltpu.make_async_copy(right_hbm.at[:, rest], right_ref.at[:, rest], sem.at[0])
    left_load = pltpu.make_async_copy(left_hbm, left_ref, sem.at[1])
    right_load.start()
    left_load.start()
    return right_load, left_load


def mix(rows_ref, first_ref, right_ref, mixed_ref, tile, loads):
    for start in range(0, mixed_ref.shape[1], tile):
        cols = pl.ds(start, tile)
        if start == tile:
            loads[0].wait()
        columns = right_ref[:, cols] if start > 0 else first_ref[...]
        mixed = jnp.dot(rows_ref[...], columns, preferred_element_type=jnp.float32)
        mixed_ref[:, cols] = mixed.astype(jnp.bfloat16)
    loads[1].wait()


def own_block(rows_in, first, right, left, table, half, parts=()):
    block_size = right.shape[0]
    shape = (block_size, block_size)
    square = pltpu.VMEM(shape, jnp.bfloat16)
    finished = len(parts) > 0
    if finished:
        kernel, held = block_kernel, pltpu.VMEM(shape, jnp.float32)
        out_shape = jax.ShapeDtypeStruct(shape, jnp.bfloat16)
    else:
        kernel, held = raw_block_kernel, square
        out_shape = (pltpu.HBM(shape, jnp.bfloat16), jax.ShapeDtypeStruct((1, table[0].size), jnp.float32))
    return pl.pallas_call(
        functools.partial(kernel, half),
        out_shape=out_shape,
        in_specs=[VMEM] * (len(parts) + 3) + [HBM] * 2,
        out_specs=VMEM if finished else (HBM, VMEM),
        scratch_shapes=[square, square, square, held, pltpu.SemaphoreType.DMA((2,))],
        compiler_params=pltpu.CompilerParams(vmem_limit_bytes=24 * MIB),
        name="own_block" if finished else "raw_block",
        cost_estimate=pl.CostEstimate(
            flops=4 * block_size**3, bytes_accessed=8 * block_size**2, transcendentals=0
        ),
    )(table, *parts, rows_in, first, in_hbm(right), in_hbm(left))


def exchange(value):
    return lax.all_to_all(value, DP, split_axis=0, concat_axis=0, tiled=True)


def adam_sums(grad, second_moment, block_size):
    row_blocks, block_rows, half_cols = grad.shape
    col_blocks = half_cols // block_size
    widened = grad.astype(jnp.float32)
    square = widened * widened
    moment_new = BETA_TWO * second_moment + (1.0 - BETA_TWO) * square
    root = moment_new * lax.rsqrt(moment_new)
    ratio = square / (moment_new + ADAM_EPS * (2.0 * root + ADAM_EPS))
    sums = jnp.sum(ratio.reshape(row_blocks, block_rows, col_blocks, block_size), axis=(1, 3))
    return jnp.transpose(sums).reshape(1, row_blocks * col_blocks)


def plane_sums(value):
    return lax.psum(lax.psum(value, "dp_0"), "dp_2")


def all_shifts(value, axis):
    size = lax.axis_size(axis)
    values = [value]
    for step in range(1, size):
        ring = [(i, (i + step) % size) for i in range(size)]
        values.append(lax.ppermute(value, axis, ring))
    return values


def all_planes(plane):
    return all_shifts(plane, "dp_1")


def first_core(grad, second_moment, left, right, table):
    block_size = left.shape[0]
    slots = lax.axis_size(DP)
    outgoing, first = gather_rows(table, grad, 1, slots, block_size, right)
    rows_in = exchange(outgoing)
    result, square = own_block(
        rows_in.reshape(block_size, block_size), first, right, left, table, 1
    )
    second_moment, result = lax.optimization_barrier((second_moment, result))
    back = exchange(result.reshape(outgoing.shape))
    sums = jnp.concatenate([adam_sums(grad, second_moment, block_size), square], axis=0)
    return scatter_rows(table, back, 1, grad, all_planes(plane_sums(sums)))


def second_core(grad, second_moment, left, right, table):
    block_size = left.shape[0]
    outgoing = gather_rows(table, grad, 0, lax.axis_size(DP), block_size)
    sums = sum(all_shifts(adam_sums(grad, second_moment, block_size), "dp_0"))
    parts = all_planes(sum(all_shifts(sums, "dp_2")))
    first = fetch_columns(parts[0], right, block_size // 2)
    first, *parts[:1], outgoing = lax.optimization_barrier((first, *parts[:1], outgoing))
    rows_in = exchange(outgoing)
    result = own_block(
        rows_in.reshape(block_size, block_size), first, right, left, table, 0, parts
    )
    back = exchange(result.reshape(outgoing.shape))
    return scatter_rows(table, back, 0, grad)


def per_device(grad, second_moment, left_root, right_root, owner_slot):
    table = jnp.transpose(owner_slot, (0, 2, 1))
    return lax.cond(
        lax.axis_index("mp") == 1,
        first_core,
        second_core,
        grad,
        second_moment,
        left_root[0, 0],
        right_root[0, 0],
        table,
    )


def solution(mesh):
    split = Mesh(mesh.devices.reshape(4, 8, 4, mesh.shape["mp"]), ("dp_0", "dp_1", "dp_2", "mp"))
    return jax.shard_map(
        per_device,
        mesh=split,
        in_specs=(
            P(None, DP, "mp"),
            P(None, DP, "mp"),
            P("mp", DP, None, None),
            P("mp", DP, None, None),
            P(),
        ),
        out_specs=P(None, DP, "mp"),
        check_vma=False,
    )
```

```python
import functools

import jax
import jax.numpy as jnp
from jax import lax
from jax.experimental import pallas as pl
from jax.experimental.pallas import tpu as pltpu
from jax.sharding import Mesh
from jax.sharding import PartitionSpec as P

Z = ("z_2", "z_1", "z_0")
DP = ("dp_0", *Z, "dp_2")
SPREAD = ("dp_0", "dp_2", "z_0", "z_1", "z_2")


BETA_TWO = 0.99
ADAM_EPS = 1e-08
NORM_EPS = 1e-06
MIB = 1 << 20
VMEM = pl.BlockSpec(memory_space=pltpu.VMEM)
HBM = pl.BlockSpec(memory_space=pltpu.HBM)
SMEM = pl.BlockSpec(memory_space=pltpu.SMEM)


def in_hbm(value):
    return pltpu.with_memory_space_constraint(value, pltpu.HBM)


def spread(slot):
    z_0, z_1, z_2 = (slot >> 2) & 1, (slot >> 3) & 1, (slot >> 4) & 1
    return (slot & 96) | ((slot & 3) << 3) | (z_0 << 2) | (z_1 << 1) | z_2


def gather_kernel(groups, half, table_hbm, grad_hbm, *refs):
    in_vmem = len(refs) > 6
    if in_vmem:
        right_hbm, out_ref, first_ref, table_ref, held_ref, table_sem, in_sem, out_sem = refs
    else:
        out_ref, table_ref, held_ref, table_sem, in_sem, out_sem = refs
    row_blocks = grad_hbm.shape[0]
    block_size = out_ref.shape[-1]
    col_blocks = grad_hbm.shape[2] // block_size
    group = row_blocks // groups

    def load(g):
        rows = pl.ds(g * group, group)
        return pltpu.make_async_copy(grad_hbm.at[rows], held_ref.at[rows], in_sem.at[g])

    table_load = pltpu.make_async_copy(table_hbm, table_ref, table_sem)
    table_load.start()
    for g in range(groups):
        load(g).start()
    if in_vmem:
        columns = right_hbm.at[:, pl.ds(0, first_ref.shape[1])]
        first_load = pltpu.make_async_copy(columns, first_ref, out_sem)
        first_load.start()
    table_load.wait()
    for g in range(groups):
        load(g).wait()

        def one_row(row, carry):
            for col in range(col_blocks):
                columns = pl.ds(col * block_size, block_size)
                slot = table_ref[half, col, row]
                if in_vmem:
                    out_ref[slot] = held_ref[row, :, columns]
                else:
                    pltpu.make_async_copy(held_ref.at[row, :, columns], out_ref.at[spread(slot)], out_sem).start()
            return carry

        lax.fori_loop(g * group, (g + 1) * group, one_row, 0)
    if in_vmem:
        first_load.wait()
    else:
        pltpu.make_async_copy(out_ref, out_ref, out_sem).wait()


def gather_rows(table, grad, half, slots, block_size, right=None):
    groups = 8
    shape = (slots, grad.shape[1], block_size)
    in_vmem = right is not None
    if in_vmem:
        rows = jax.ShapeDtypeStruct(shape, jnp.bfloat16)
        out_shape = (rows, jax.ShapeDtypeStruct((block_size, block_size // 2), jnp.bfloat16))
    else:
        out_shape = pltpu.HBM(shape, jnp.bfloat16)
    return pl.pallas_call(
        functools.partial(gather_kernel, groups, half),
        out_shape=out_shape,
        in_specs=[HBM, HBM] + [HBM] * in_vmem,
        out_specs=(VMEM, VMEM) if in_vmem else HBM,
        scratch_shapes=[
            pltpu.SMEM(table.shape, jnp.int32),
            pltpu.VMEM(grad.shape, jnp.bfloat16),
            pltpu.SemaphoreType.DMA,
            pltpu.SemaphoreType.DMA((groups,)),
            pltpu.SemaphoreType.DMA,
        ],
        compiler_params=pltpu.CompilerParams(vmem_limit_bytes=12 * MIB),
        name="gather_rows",
    )(in_hbm(table), in_hbm(grad), *([in_hbm(right)] if in_vmem else []))


def scatter_kernel(half, table_ref, back_ref, out_ref, held_ref, sem):
    row_blocks = out_ref.shape[0]
    block_size = back_ref.shape[-1]
    col_blocks = out_ref.shape[2] // block_size

    def one_row(row, carry):
        for col in range(col_blocks):
            columns = pl.ds(col * block_size, block_size)
            held_ref[row, :, columns] = back_ref[spread(table_ref[half, col, row])]
        pltpu.make_async_copy(held_ref.at[row], out_ref.at[row], sem).start()
        return carry

    lax.fori_loop(0, row_blocks, one_row, 0)
    pltpu.make_async_copy(out_ref, out_ref, sem).wait()


def scaled_scatter_kernel(parts, half, table_ref, *refs):
    part_refs = refs[:parts]
    back_ref, out_ref, norm_ref, held_ref, sem = refs[parts:]
    row_blocks = out_ref.shape[0]
    block_size = back_ref.shape[-1]
    col_blocks = out_ref.shape[2] // block_size
    blocks = row_blocks * col_blocks
    totals = part_refs[0][...]
    for part_ref in part_refs[1:]:
        totals = totals + part_ref[...]
    norms = jnp.sqrt((totals[0:1] + NORM_EPS) / (totals[1:2] + NORM_EPS))
    norm_ref[...] = jnp.transpose(jnp.broadcast_to(norms, (blocks, blocks)))

    def one_row(row, carry):
        for col in range(col_blocks):
            slot = table_ref[half, col, row]
            norm = norm_ref[pl.ds(col * row_blocks + row, 1), :]
            norm = jnp.concatenate([norm] * (block_size // blocks), axis=1)
            rows = back_ref[slot].astype(jnp.float32) * norm
            held_ref[row, :, pl.ds(col * block_size, block_size)] = rows.astype(jnp.bfloat16)
        pltpu.make_async_copy(held_ref.at[row], out_ref.at[row], sem).start()
        return carry

    lax.fori_loop(0, row_blocks, one_row, 0)
    pltpu.make_async_copy(out_ref, out_ref, sem).wait()


def scatter_rows(table, back, half, like, parts=None):
    out_shape = pltpu.HBM(like.shape, jnp.bfloat16)
    params = pltpu.CompilerParams(vmem_limit_bytes=8 * MIB)
    if parts is None:
        return pl.pallas_call(
            functools.partial(scatter_kernel, half),
            out_shape=out_shape,
            in_specs=[SMEM, VMEM],
            out_specs=HBM,
            scratch_shapes=[pltpu.VMEM(like.shape, jnp.bfloat16), pltpu.SemaphoreType.DMA],
            compiler_params=params,
            name="scatter_rows",
        )(table, back)
    blocks = parts[0].shape[1]
    return pl.pallas_call(
        functools.partial(scaled_scatter_kernel, len(parts), half),
        out_shape=out_shape,
        in_specs=[SMEM] + [VMEM] * (len(parts) + 1),
        out_specs=HBM,
        scratch_shapes=[
            pltpu.VMEM((blocks, blocks), jnp.float32),
            pltpu.VMEM(like.shape, jnp.bfloat16),
            pltpu.SemaphoreType.DMA,
        ],
        compiler_params=params,
        name="scaled_scatter_rows",
    )(table, *parts, back)


def fetch_kernel(after_ref, right_hbm, out_ref, sem):
    columns = right_hbm.at[:, pl.ds(0, out_ref.shape[1])]
    copy = pltpu.make_async_copy(columns, out_ref, sem)
    copy.start()
    copy.wait()


def fetch_columns(after, right, columns):
    return pl.pallas_call(
        fetch_kernel,
        out_shape=jax.ShapeDtypeStruct((right.shape[0], columns), jnp.bfloat16),
        in_specs=[VMEM, HBM],
        out_specs=VMEM,
        scratch_shapes=[pltpu.SemaphoreType.DMA],
        compiler_params=pltpu.CompilerParams(vmem_limit_bytes=8 * MIB),
        name="fetch_columns",
    )(after, in_hbm(right))


def owners(table_ref, half):
    table = table_ref[half]
    return jnp.concatenate([table[col : col + 1] for col in range(table.shape[0])], axis=1)


def block_kernel(half, table_ref, *refs):
    parts = len(refs) - 10
    part_refs = refs[:parts]
    rows_ref, first_ref, right_hbm, left_hbm, out_ref, right_ref, left_ref, mixed_ref, shaped_ref, sem = refs[parts:]
    block_size = right_hbm.shape[0]
    tile = first_ref.shape[1]
    loads = start_loads(right_hbm, left_hbm, right_ref, left_ref, tile, sem)
    totals = part_refs[0][...]
    for part_ref in part_refs[1:]:
        totals = totals + part_ref[...]
    adam_sq = jnp.sum(jnp.where(owners(table_ref, half) == lax.axis_index(DP), totals, 0.0))
    places = [spread(slot) for slot in range(lax.axis_size(DP))]
    mix(rows_ref, first_ref, right_ref, mixed_ref, tile, loads, places)

    def shape(j, squares):
        cols = pl.ds(pl.multiple_of(j * tile, tile), tile)
        shaped = jnp.dot(left_ref[...], mixed_ref[:, cols], preferred_element_type=jnp.float32)
        shaped_ref[:, cols] = shaped
        return squares + jnp.sum((shaped * shaped).reshape(block_size // 8, 8, tile), axis=0)

    squares = lax.fori_loop(0, block_size // tile, shape, jnp.zeros((8, tile), jnp.float32))
    shaped_sq = jnp.full((8, 128), jnp.sum(squares), jnp.float32)
    scale = jnp.sqrt((adam_sq + NORM_EPS) / (shaped_sq + NORM_EPS))[0:1, 0:1]
    each = block_size // len(places)
    for group, place in enumerate(places):
        rows = shaped_ref[pl.ds(group * each, each), :] * scale
        out_ref[pl.ds(place * each, each), :] = rows.astype(jnp.bfloat16)


def raw_block_kernel(
    half, table_ref, rows_ref, first_ref, right_hbm, left_hbm, out_hbm, square_ref, right_ref, left_ref, mixed_ref, held_ref, sem
):
    block_size = right_hbm.shape[0]
    tile = first_ref.shape[1]
    steps = block_size // tile
    loads = start_loads(right_hbm, left_hbm, right_ref, left_ref, tile, sem)
    mix(rows_ref, first_ref, right_ref, mixed_ref, tile, loads)

    def store(j):
        cols = pl.ds(pl.multiple_of(j * tile, tile), tile)
        return pltpu.make_async_copy(held_ref.at[:, cols], out_hbm.at[:, cols], sem.at[j])

    def shape(j, squares):
        cols = pl.ds(pl.multiple_of(j * tile, tile), tile)
        shaped = jnp.dot(left_ref[...], mixed_ref[:, cols], preferred_element_type=jnp.float32)
        held_ref[:, cols] = shaped.astype(jnp.bfloat16)
        store(j).start()
        return squares + jnp.sum((shaped * shaped).reshape(block_size // 8, 8, tile), axis=0)

    squares = lax.fori_loop(0, steps, shape, jnp.zeros((8, tile), jnp.float32))
    square_ref[...] = jnp.where(owners(table_ref, half) == lax.axis_index(DP), jnp.sum(squares), 0.0)
    for j in range(steps):
        store(j).wait()


def start_loads(right_hbm, left_hbm, right_ref, left_ref, tile, sem):
    rest = pl.ds(tile, right_hbm.shape[1] - tile)
    right_load = pltpu.make_async_copy(right_hbm.at[:, rest], right_ref.at[:, rest], sem.at[0])
    left_load = pltpu.make_async_copy(left_hbm, left_ref, sem.at[1])
    right_load.start()
    left_load.start()
    return right_load, left_load


def mix(rows_ref, first_ref, right_ref, mixed_ref, tile, loads, places=None):
    for start in range(0, mixed_ref.shape[1], tile):
        cols = pl.ds(start, tile)
        if start == tile:
            loads[0].wait()
        columns = right_ref[:, cols] if start > 0 else first_ref[...]
        mixed = jnp.dot(rows_ref[...], columns, preferred_element_type=jnp.float32)
        mixed = mixed.astype(jnp.bfloat16)
        if places is None:
            mixed_ref[:, cols] = mixed
        else:
            each = mixed.shape[0] // len(places)
            for group, place in enumerate(places):
                mixed_ref[pl.ds(group * each, each), cols] = mixed[place * each : (place + 1) * each]
    loads[1].wait()


def own_block(rows_in, first, right, left, table, half, parts=()):
    block_size = right.shape[0]
    shape = (block_size, block_size)
    square = pltpu.VMEM(shape, jnp.bfloat16)
    finished = len(parts) > 0
    if finished:
        kernel, held = block_kernel, pltpu.VMEM(shape, jnp.float32)
        out_shape = jax.ShapeDtypeStruct(shape, jnp.bfloat16)
    else:
        kernel, held = raw_block_kernel, square
        out_shape = (pltpu.HBM(shape, jnp.bfloat16), jax.ShapeDtypeStruct((1, table[0].size), jnp.float32))
    return pl.pallas_call(
        functools.partial(kernel, half),
        out_shape=out_shape,
        in_specs=[VMEM] * (len(parts) + 3) + [HBM] * 2,
        out_specs=VMEM if finished else (HBM, VMEM),
        scratch_shapes=[square, square, square, held, pltpu.SemaphoreType.DMA((2,))],
        compiler_params=pltpu.CompilerParams(vmem_limit_bytes=24 * MIB),
        name="own_block" if finished else "raw_block",
        cost_estimate=pl.CostEstimate(
            flops=4 * block_size**3, bytes_accessed=8 * block_size**2, transcendentals=0
        ),
    )(table, *parts, rows_in, first, in_hbm(right), in_hbm(left))


def exchange(value, axes=DP):
    return lax.all_to_all(value, axes, split_axis=0, concat_axis=0, tiled=True)


def adam_sums(grad, second_moment, block_size):
    row_blocks, block_rows, half_cols = grad.shape
    col_blocks = half_cols // block_size
    widened = grad.astype(jnp.float32)
    square = widened * widened
    moment_new = BETA_TWO * second_moment + (1.0 - BETA_TWO) * square
    root = moment_new * lax.rsqrt(moment_new)
    ratio = square / (moment_new + ADAM_EPS * (2.0 * root + ADAM_EPS))
    sums = jnp.sum(ratio.reshape(row_blocks, block_rows, col_blocks, block_size), axis=(1, 3))
    return jnp.transpose(sums).reshape(1, row_blocks * col_blocks)


def plane_sums(value):
    return lax.psum(lax.psum(value, "dp_0"), "dp_2")


def all_shifts(value, axis):
    size = lax.axis_size(axis)
    values = [value]
    for step in range(1, size):
        ring = [(i, (i + step) % size) for i in range(size)]
        values.append(lax.ppermute(value, axis, ring))
    return values


def all_planes(plane):
    return all_shifts(plane, Z)


def first_core(grad, second_moment, left, right, table):
    block_size = left.shape[0]
    slots = lax.axis_size(DP)
    outgoing, first = gather_rows(table, grad, 1, slots, block_size, right)
    rows_in = exchange(outgoing)
    result, square = own_block(
        rows_in.reshape(block_size, block_size), first, right, left, table, 1
    )
    second_moment, result = lax.optimization_barrier((second_moment, result))
    back = exchange(result.reshape(outgoing.shape))
    sums = jnp.concatenate([adam_sums(grad, second_moment, block_size), square], axis=0)
    return scatter_rows(table, back, 1, grad, all_planes(plane_sums(sums)))


def second_core(grad, second_moment, left, right, table):
    block_size = left.shape[0]
    outgoing = gather_rows(table, grad, 0, lax.axis_size(DP), block_size)
    sums = sum(all_shifts(adam_sums(grad, second_moment, block_size), "dp_0"))
    parts = all_planes(sum(all_shifts(sums, "dp_2")))
    first = fetch_columns(parts[0], right, block_size // 2)
    first, *parts[:1], outgoing = lax.optimization_barrier((first, *parts[:1], outgoing))
    rows_in = exchange(outgoing, SPREAD)
    result = own_block(
        rows_in.reshape(block_size, block_size), first, right, left, table, 0, parts
    )
    back = exchange(result.reshape(outgoing.shape), SPREAD)
    return scatter_rows(table, back, 0, grad)


def per_device(grad, second_moment, left_root, right_root, owner_slot):
    table = jnp.transpose(owner_slot, (0, 2, 1))
    return lax.cond(
        lax.axis_index("mp") == 1,
        first_core,
        second_core,
        grad,
        second_moment,
        left_root[0, 0],
        right_root[0, 0],
        table,
    )


def solution(mesh):
    split = Mesh(mesh.devices.reshape(4, 2, 2, 2, 4, mesh.shape["mp"]), ("dp_0", *Z, "dp_2", "mp"))
    return jax.shard_map(
        per_device,
        mesh=split,
        in_specs=(
            P(None, DP, "mp"),
            P(None, DP, "mp"),
            P("mp", DP, None, None),
            P("mp", DP, None, None),
            P(),
        ),
        out_specs=P(None, DP, "mp"),
        check_vma=False,
    )
```

```python
import functools

import jax
import jax.numpy as jnp
from jax import lax
from jax.experimental import pallas as pl
from jax.experimental.pallas import tpu as pltpu
from jax.sharding import Mesh
from jax.sharding import PartitionSpec as P

Z = ("z_2", "z_1", "z_0")
DP = ("dp_0", *Z, "dp_2")
SPREAD = ("dp_0", "dp_2", "z_0", "z_1", "z_2")


BETA_TWO = 0.99
ADAM_EPS = 1e-08
NORM_EPS = 1e-06
MIB = 1 << 20
VMEM = pl.BlockSpec(memory_space=pltpu.VMEM)
HBM = pl.BlockSpec(memory_space=pltpu.HBM)
SMEM = pl.BlockSpec(memory_space=pltpu.SMEM)


def in_hbm(value):
    return pltpu.with_memory_space_constraint(value, pltpu.HBM)


def spread(slot):
    z_0, z_1, z_2 = (slot >> 2) & 1, (slot >> 3) & 1, (slot >> 4) & 1
    return (slot & 96) | ((slot & 3) << 3) | (z_0 << 2) | (z_1 << 1) | z_2


def gather_kernel(groups, half, table_hbm, grad_hbm, *refs):
    in_vmem = len(refs) > 6
    if in_vmem:
        right_hbm, out_ref, first_ref, table_ref, held_ref, table_sem, in_sem, out_sem = refs
    else:
        out_ref, table_ref, held_ref, table_sem, in_sem, out_sem = refs
    row_blocks = grad_hbm.shape[0]
    block_size = out_ref.shape[-1]
    col_blocks = grad_hbm.shape[2] // block_size
    group = row_blocks // groups

    def load(g):
        rows = pl.ds(g * group, group)
        return pltpu.make_async_copy(grad_hbm.at[rows], held_ref.at[rows], in_sem.at[g])

    table_load = pltpu.make_async_copy(table_hbm, table_ref, table_sem)
    table_load.start()
    for g in range(groups):
        load(g).start()
    if in_vmem:
        columns = right_hbm.at[:, pl.ds(0, first_ref.shape[1])]
        first_load = pltpu.make_async_copy(columns, first_ref, out_sem)
        first_load.start()
    table_load.wait()
    for g in range(groups):
        load(g).wait()

        def one_row(row, carry):
            for col in range(col_blocks):
                columns = pl.ds(col * block_size, block_size)
                slot = table_ref[half, col, row]
                if in_vmem:
                    out_ref[slot] = held_ref[row, :, columns]
                else:
                    pltpu.make_async_copy(held_ref.at[row, :, columns], out_ref.at[spread(slot)], out_sem).start()
            return carry

        lax.fori_loop(g * group, (g + 1) * group, one_row, 0, unroll=4)
    if in_vmem:
        first_load.wait()
    else:
        pltpu.make_async_copy(out_ref, out_ref, out_sem).wait()


def gather_rows(table, grad, half, slots, block_size, right=None):
    groups = 8
    shape = (slots, grad.shape[1], block_size)
    in_vmem = right is not None
    if in_vmem:
        rows = jax.ShapeDtypeStruct(shape, jnp.bfloat16)
        out_shape = (rows, jax.ShapeDtypeStruct((block_size, block_size // 2), jnp.bfloat16))
    else:
        out_shape = pltpu.HBM(shape, jnp.bfloat16)
    return pl.pallas_call(
        functools.partial(gather_kernel, groups, half),
        out_shape=out_shape,
        in_specs=[HBM, HBM] + [HBM] * in_vmem,
        out_specs=(VMEM, VMEM) if in_vmem else HBM,
        scratch_shapes=[
            pltpu.SMEM(table.shape, jnp.int32),
            pltpu.VMEM(grad.shape, jnp.bfloat16),
            pltpu.SemaphoreType.DMA,
            pltpu.SemaphoreType.DMA((groups,)),
            pltpu.SemaphoreType.DMA,
        ],
        compiler_params=pltpu.CompilerParams(vmem_limit_bytes=12 * MIB),
        name="gather_rows",
    )(in_hbm(table), in_hbm(grad), *([in_hbm(right)] if in_vmem else []))


def scatter_kernel(half, table_ref, back_ref, out_ref, held_ref, sem):
    row_blocks = out_ref.shape[0]
    block_size = back_ref.shape[-1]
    col_blocks = out_ref.shape[2] // block_size

    def one_row(row, carry):
        for col in range(col_blocks):
            columns = pl.ds(col * block_size, block_size)
            held_ref[row, :, columns] = back_ref[spread(table_ref[half, col, row])]
        pltpu.make_async_copy(held_ref.at[row], out_ref.at[row], sem).start()
        return carry

    lax.fori_loop(0, row_blocks, one_row, 0)
    pltpu.make_async_copy(out_ref, out_ref, sem).wait()


def scaled_scatter_kernel(parts, half, table_ref, *refs):
    part_refs = refs[:parts]
    back_ref, out_ref, norm_ref, held_ref, sem = refs[parts:]
    row_blocks = out_ref.shape[0]
    block_size = back_ref.shape[-1]
    col_blocks = out_ref.shape[2] // block_size
    blocks = row_blocks * col_blocks
    totals = part_refs[0][...]
    for part_ref in part_refs[1:]:
        totals = totals + part_ref[...]
    norms = jnp.sqrt((totals[0:1] + NORM_EPS) / (totals[1:2] + NORM_EPS))
    norm_ref[...] = jnp.transpose(jnp.broadcast_to(norms, (blocks, blocks)))

    def one_row(row, carry):
        for col in range(col_blocks):
            slot = table_ref[half, col, row]
            norm = norm_ref[pl.ds(col * row_blocks + row, 1), :]
            norm = jnp.concatenate([norm] * (block_size // blocks), axis=1)
            rows = back_ref[slot].astype(jnp.float32) * norm
            held_ref[row, :, pl.ds(col * block_size, block_size)] = rows.astype(jnp.bfloat16)
        pltpu.make_async_copy(held_ref.at[row], out_ref.at[row], sem).start()
        return carry

    lax.fori_loop(0, row_blocks, one_row, 0)
    pltpu.make_async_copy(out_ref, out_ref, sem).wait()


def scatter_rows(table, back, half, like, parts=None):
    out_shape = pltpu.HBM(like.shape, jnp.bfloat16)
    params = pltpu.CompilerParams(vmem_limit_bytes=8 * MIB)
    if parts is None:
        return pl.pallas_call(
            functools.partial(scatter_kernel, half),
            out_shape=out_shape,
            in_specs=[SMEM, VMEM],
            out_specs=HBM,
            scratch_shapes=[pltpu.VMEM(like.shape, jnp.bfloat16), pltpu.SemaphoreType.DMA],
            compiler_params=params,
            name="scatter_rows",
        )(table, back)
    blocks = parts[0].shape[1]
    return pl.pallas_call(
        functools.partial(scaled_scatter_kernel, len(parts), half),
        out_shape=out_shape,
        in_specs=[SMEM] + [VMEM] * (len(parts) + 1),
        out_specs=HBM,
        scratch_shapes=[
            pltpu.VMEM((blocks, blocks), jnp.float32),
            pltpu.VMEM(like.shape, jnp.bfloat16),
            pltpu.SemaphoreType.DMA,
        ],
        compiler_params=params,
        name="scaled_scatter_rows",
    )(table, *parts, back)


def fetch_kernel(after_ref, right_hbm, out_ref, sem):
    columns = right_hbm.at[:, pl.ds(0, out_ref.shape[1])]
    copy = pltpu.make_async_copy(columns, out_ref, sem)
    copy.start()
    copy.wait()


def fetch_columns(after, right, columns):
    return pl.pallas_call(
        fetch_kernel,
        out_shape=jax.ShapeDtypeStruct((right.shape[0], columns), jnp.bfloat16),
        in_specs=[VMEM, HBM],
        out_specs=VMEM,
        scratch_shapes=[pltpu.SemaphoreType.DMA],
        compiler_params=pltpu.CompilerParams(vmem_limit_bytes=8 * MIB),
        name="fetch_columns",
    )(after, in_hbm(right))


def owners(table_ref, half):
    table = table_ref[half]
    return jnp.concatenate([table[col : col + 1] for col in range(table.shape[0])], axis=1)


def block_kernel(half, table_ref, *refs):
    parts = len(refs) - 10
    part_refs = refs[:parts]
    rows_ref, first_ref, right_hbm, left_hbm, out_ref, right_ref, left_ref, mixed_ref, shaped_ref, sem = refs[parts:]
    block_size = right_hbm.shape[0]
    tile = first_ref.shape[1]
    loads = start_loads(right_hbm, left_hbm, right_ref, left_ref, tile, sem)
    totals = part_refs[0][...]
    for part_ref in part_refs[1:]:
        totals = totals + part_ref[...]
    adam_sq = jnp.sum(jnp.where(owners(table_ref, half) == lax.axis_index(DP), totals, 0.0))
    places = [spread(slot) for slot in range(lax.axis_size(DP))]
    mix(rows_ref, first_ref, right_ref, mixed_ref, tile, loads, places)

    def shape(j, squares):
        cols = pl.ds(pl.multiple_of(j * tile, tile), tile)
        shaped = jnp.dot(left_ref[...], mixed_ref[:, cols], preferred_element_type=jnp.float32)
        shaped_ref[:, cols] = shaped
        return squares + jnp.sum((shaped * shaped).reshape(block_size // 8, 8, tile), axis=0)

    squares = lax.fori_loop(0, block_size // tile, shape, jnp.zeros((8, tile), jnp.float32))
    shaped_sq = jnp.full((8, 128), jnp.sum(squares), jnp.float32)
    scale = jnp.sqrt((adam_sq + NORM_EPS) / (shaped_sq + NORM_EPS))[0:1, 0:1]
    each = block_size // len(places)
    for group, place in enumerate(places):
        rows = shaped_ref[pl.ds(group * each, each), :] * scale
        out_ref[pl.ds(place * each, each), :] = rows.astype(jnp.bfloat16)


def raw_block_kernel(
    half, table_ref, rows_ref, first_ref, right_hbm, left_hbm, out_hbm, square_ref, right_ref, left_ref, mixed_ref, held_ref, sem
):
    block_size = right_hbm.shape[0]
    tile = first_ref.shape[1]
    steps = block_size // tile
    loads = start_loads(right_hbm, left_hbm, right_ref, left_ref, tile, sem)
    mix(rows_ref, first_ref, right_ref, mixed_ref, tile, loads)

    def store(j):
        cols = pl.ds(pl.multiple_of(j * tile, tile), tile)
        return pltpu.make_async_copy(held_ref.at[:, cols], out_hbm.at[:, cols], sem.at[j])

    def shape(j, squares):
        cols = pl.ds(pl.multiple_of(j * tile, tile), tile)
        shaped = jnp.dot(left_ref[...], mixed_ref[:, cols], preferred_element_type=jnp.float32)
        held_ref[:, cols] = shaped.astype(jnp.bfloat16)
        store(j).start()
        return squares + jnp.sum((shaped * shaped).reshape(block_size // 8, 8, tile), axis=0)

    squares = lax.fori_loop(0, steps, shape, jnp.zeros((8, tile), jnp.float32))
    square_ref[...] = jnp.where(owners(table_ref, half) == lax.axis_index(DP), jnp.sum(squares), 0.0)
    for j in range(steps):
        store(j).wait()


def start_loads(right_hbm, left_hbm, right_ref, left_ref, tile, sem):
    rest = pl.ds(tile, right_hbm.shape[1] - tile)
    right_load = pltpu.make_async_copy(right_hbm.at[:, rest], right_ref.at[:, rest], sem.at[0])
    left_load = pltpu.make_async_copy(left_hbm, left_ref, sem.at[1])
    right_load.start()
    left_load.start()
    return right_load, left_load


def mix(rows_ref, first_ref, right_ref, mixed_ref, tile, loads, places=None):
    for start in range(0, mixed_ref.shape[1], tile):
        cols = pl.ds(start, tile)
        if start == tile:
            loads[0].wait()
        columns = right_ref[:, cols] if start > 0 else first_ref[...]
        mixed = jnp.dot(rows_ref[...], columns, preferred_element_type=jnp.float32)
        mixed = mixed.astype(jnp.bfloat16)
        if places is None:
            mixed_ref[:, cols] = mixed
        else:
            each = mixed.shape[0] // len(places)
            for group, place in enumerate(places):
                mixed_ref[pl.ds(group * each, each), cols] = mixed[place * each : (place + 1) * each]
    loads[1].wait()


def own_block(rows_in, first, right, left, table, half, parts=()):
    block_size = right.shape[0]
    shape = (block_size, block_size)
    square = pltpu.VMEM(shape, jnp.bfloat16)
    finished = len(parts) > 0
    if finished:
        kernel, held = block_kernel, pltpu.VMEM(shape, jnp.float32)
        out_shape = jax.ShapeDtypeStruct(shape, jnp.bfloat16)
    else:
        kernel, held = raw_block_kernel, square
        out_shape = (pltpu.HBM(shape, jnp.bfloat16), jax.ShapeDtypeStruct((1, table[0].size), jnp.float32))
    return pl.pallas_call(
        functools.partial(kernel, half),
        out_shape=out_shape,
        in_specs=[VMEM] * (len(parts) + 3) + [HBM] * 2,
        out_specs=VMEM if finished else (HBM, VMEM),
        scratch_shapes=[square, square, square, held, pltpu.SemaphoreType.DMA((2,))],
        compiler_params=pltpu.CompilerParams(vmem_limit_bytes=24 * MIB),
        name="own_block" if finished else "raw_block",
        cost_estimate=pl.CostEstimate(
            flops=4 * block_size**3, bytes_accessed=8 * block_size**2, transcendentals=0
        ),
    )(table, *parts, rows_in, first, in_hbm(right), in_hbm(left))


def exchange(value, axes=DP):
    return lax.all_to_all(value, axes, split_axis=0, concat_axis=0, tiled=True)


def adam_sums(grad, second_moment, block_size):
    row_blocks, block_rows, half_cols = grad.shape
    col_blocks = half_cols // block_size
    widened = grad.astype(jnp.float32)
    square = widened * widened
    moment_new = BETA_TWO * second_moment + (1.0 - BETA_TWO) * square
    root = moment_new * lax.rsqrt(moment_new)
    ratio = square / (moment_new + ADAM_EPS * (2.0 * root + ADAM_EPS))
    sums = jnp.sum(ratio.reshape(row_blocks, block_rows, col_blocks, block_size), axis=(1, 3))
    return jnp.transpose(sums).reshape(1, row_blocks * col_blocks)


def plane_sums(value):
    return lax.psum(lax.psum(value, "dp_0"), "dp_2")


def all_shifts(value, axis):
    size = lax.axis_size(axis)
    values = [value]
    for step in range(1, size):
        ring = [(i, (i + step) % size) for i in range(size)]
        values.append(lax.ppermute(value, axis, ring))
    return values


def all_planes(plane):
    return all_shifts(plane, Z)


def first_core(grad, second_moment, left, right, table):
    block_size = left.shape[0]
    slots = lax.axis_size(DP)
    outgoing, first = gather_rows(table, grad, 1, slots, block_size, right)
    rows_in = exchange(outgoing)
    result, square = own_block(
        rows_in.reshape(block_size, block_size), first, right, left, table, 1
    )
    second_moment, result = lax.optimization_barrier((second_moment, result))
    back = exchange(result.reshape(outgoing.shape))
    sums = jnp.concatenate([adam_sums(grad, second_moment, block_size), square], axis=0)
    return scatter_rows(table, back, 1, grad, all_planes(plane_sums(sums)))


def second_core(grad, second_moment, left, right, table):
    block_size = left.shape[0]
    outgoing = gather_rows(table, grad, 0, lax.axis_size(DP), block_size)
    sums = sum(all_shifts(adam_sums(grad, second_moment, block_size), "dp_0"))
    parts = all_planes(sum(all_shifts(sums, "dp_2")))
    first = fetch_columns(parts[0], right, block_size // 2)
    first, *parts[:1], outgoing = lax.optimization_barrier((first, *parts[:1], outgoing))
    rows_in = exchange(outgoing, SPREAD)
    result = own_block(
        rows_in.reshape(block_size, block_size), first, right, left, table, 0, parts
    )
    back = exchange(result.reshape(outgoing.shape), SPREAD)
    return scatter_rows(table, back, 0, grad)


def per_device(grad, second_moment, left_root, right_root, owner_slot):
    table = jnp.transpose(owner_slot, (0, 2, 1))
    return lax.cond(
        lax.axis_index("mp") == 1,
        first_core,
        second_core,
        grad,
        second_moment,
        left_root[0, 0],
        right_root[0, 0],
        table,
    )


def solution(mesh):
    split = Mesh(mesh.devices.reshape(4, 2, 2, 2, 4, mesh.shape["mp"]), ("dp_0", *Z, "dp_2", "mp"))
    return jax.shard_map(
        per_device,
        mesh=split,
        in_specs=(
            P(None, DP, "mp"),
            P(None, DP, "mp"),
            P("mp", DP, None, None),
            P("mp", DP, None, None),
            P(),
        ),
        out_specs=P(None, DP, "mp"),
        check_vma=False,
    )
```

```python
import functools

import jax
import jax.numpy as jnp
from jax import lax
from jax.experimental import pallas as pl
from jax.experimental.pallas import tpu as pltpu
from jax.sharding import Mesh
from jax.sharding import PartitionSpec as P

Z = ("z_2", "z_1", "z_0")
DP = ("dp_0", *Z, "dp_2")
SPREAD = ("dp_0", "dp_2", "z_0", "z_1", "z_2")


BETA_TWO = 0.99
ADAM_EPS = 1e-08
NORM_EPS = 1e-06
MIB = 1 << 20
VMEM = pl.BlockSpec(memory_space=pltpu.VMEM)
HBM = pl.BlockSpec(memory_space=pltpu.HBM)
SMEM = pl.BlockSpec(memory_space=pltpu.SMEM)


def in_hbm(value):
    return pltpu.with_memory_space_constraint(value, pltpu.HBM)


def spread(slot):
    z_0, z_1, z_2 = (slot >> 2) & 1, (slot >> 3) & 1, (slot >> 4) & 1
    return (slot & 96) | ((slot & 3) << 3) | (z_0 << 2) | (z_1 << 1) | z_2


def gather_kernel(groups, half, table_hbm, grad_hbm, *refs):
    in_vmem = len(refs) > 6
    if in_vmem:
        right_hbm, out_ref, first_ref, table_ref, held_ref, table_sem, in_sem, out_sem = refs
    else:
        out_ref, table_ref, held_ref, table_sem, in_sem, out_sem = refs
    row_blocks = grad_hbm.shape[0]
    block_size = out_ref.shape[-1]
    col_blocks = grad_hbm.shape[2] // block_size
    group = row_blocks // groups

    def load(g):
        rows = pl.ds(g * group, group)
        return pltpu.make_async_copy(grad_hbm.at[rows], held_ref.at[rows], in_sem.at[g])

    table_load = pltpu.make_async_copy(table_hbm, table_ref, table_sem)
    table_load.start()
    for g in range(groups):
        load(g).start()
    if in_vmem:
        columns = right_hbm.at[:, pl.ds(0, first_ref.shape[1])]
        first_load = pltpu.make_async_copy(columns, first_ref, out_sem)
        first_load.start()
    table_load.wait()
    for g in range(groups):
        load(g).wait()

        def one_row(row, carry):
            for col in range(col_blocks):
                columns = pl.ds(col * block_size, block_size)
                slot = table_ref[half, col, row]
                if in_vmem:
                    out_ref[slot] = held_ref[row, :, columns]
                else:
                    pltpu.make_async_copy(held_ref.at[row, :, columns], out_ref.at[spread(slot)], out_sem).start()
            return carry

        lax.fori_loop(g * group, (g + 1) * group, one_row, 0, unroll=2)
    if in_vmem:
        first_load.wait()
    else:
        pltpu.make_async_copy(out_ref, out_ref, out_sem).wait()


def gather_rows(table, grad, half, slots, block_size, right=None):
    groups = 4
    shape = (slots, grad.shape[1], block_size)
    in_vmem = right is not None
    if in_vmem:
        rows = jax.ShapeDtypeStruct(shape, jnp.bfloat16)
        out_shape = (rows, jax.ShapeDtypeStruct((block_size, block_size // 2), jnp.bfloat16))
    else:
        out_shape = pltpu.HBM(shape, jnp.bfloat16)
    return pl.pallas_call(
        functools.partial(gather_kernel, groups, half),
        out_shape=out_shape,
        in_specs=[HBM, HBM] + [HBM] * in_vmem,
        out_specs=(VMEM, VMEM) if in_vmem else HBM,
        scratch_shapes=[
            pltpu.SMEM(table.shape, jnp.int32),
            pltpu.VMEM(grad.shape, jnp.bfloat16),
            pltpu.SemaphoreType.DMA,
            pltpu.SemaphoreType.DMA((groups,)),
            pltpu.SemaphoreType.DMA,
        ],
        compiler_params=pltpu.CompilerParams(vmem_limit_bytes=12 * MIB),
        name="gather_rows",
    )(in_hbm(table), in_hbm(grad), *([in_hbm(right)] if in_vmem else []))


def scatter_kernel(half, table_ref, back_ref, out_ref, held_ref, sem):
    row_blocks = out_ref.shape[0]
    block_size = back_ref.shape[-1]
    col_blocks = out_ref.shape[2] // block_size

    def one_row(row, carry):
        for col in range(col_blocks):
            columns = pl.ds(col * block_size, block_size)
            held_ref[row, :, columns] = back_ref[spread(table_ref[half, col, row])]
        pltpu.make_async_copy(held_ref.at[row], out_ref.at[row], sem).start()
        return carry

    lax.fori_loop(0, row_blocks, one_row, 0)
    pltpu.make_async_copy(out_ref, out_ref, sem).wait()


def scaled_scatter_kernel(parts, half, table_ref, *refs):
    part_refs = refs[:parts]
    back_ref, out_ref, norm_ref, held_ref, sem = refs[parts:]
    row_blocks = out_ref.shape[0]
    block_size = back_ref.shape[-1]
    col_blocks = out_ref.shape[2] // block_size
    blocks = row_blocks * col_blocks
    totals = part_refs[0][...]
    for part_ref in part_refs[1:]:
        totals = totals + part_ref[...]
    norms = jnp.sqrt((totals[0:1] + NORM_EPS) / (totals[1:2] + NORM_EPS))
    norm_ref[...] = jnp.transpose(jnp.broadcast_to(norms, (blocks, blocks)))

    def one_row(row, carry):
        for col in range(col_blocks):
            slot = table_ref[half, col, row]
            norm = norm_ref[pl.ds(col * row_blocks + row, 1), :]
            norm = jnp.concatenate([norm] * (block_size // blocks), axis=1)
            rows = back_ref[slot].astype(jnp.float32) * norm
            held_ref[row, :, pl.ds(col * block_size, block_size)] = rows.astype(jnp.bfloat16)
        pltpu.make_async_copy(held_ref.at[row], out_ref.at[row], sem).start()
        return carry

    lax.fori_loop(0, row_blocks, one_row, 0)
    pltpu.make_async_copy(out_ref, out_ref, sem).wait()


def scatter_rows(table, back, half, like, parts=None):
    out_shape = pltpu.HBM(like.shape, jnp.bfloat16)
    params = pltpu.CompilerParams(vmem_limit_bytes=8 * MIB)
    if parts is None:
        return pl.pallas_call(
            functools.partial(scatter_kernel, half),
            out_shape=out_shape,
            in_specs=[SMEM, VMEM],
            out_specs=HBM,
            scratch_shapes=[pltpu.VMEM(like.shape, jnp.bfloat16), pltpu.SemaphoreType.DMA],
            compiler_params=params,
            name="scatter_rows",
        )(table, back)
    blocks = parts[0].shape[1]
    return pl.pallas_call(
        functools.partial(scaled_scatter_kernel, len(parts), half),
        out_shape=out_shape,
        in_specs=[SMEM] + [VMEM] * (len(parts) + 1),
        out_specs=HBM,
        scratch_shapes=[
            pltpu.VMEM((blocks, blocks), jnp.float32),
            pltpu.VMEM(like.shape, jnp.bfloat16),
            pltpu.SemaphoreType.DMA,
        ],
        compiler_params=params,
        name="scaled_scatter_rows",
    )(table, *parts, back)


def fetch_kernel(after_ref, right_hbm, out_ref, sem):
    columns = right_hbm.at[:, pl.ds(0, out_ref.shape[1])]
    copy = pltpu.make_async_copy(columns, out_ref, sem)
    copy.start()
    copy.wait()


def fetch_columns(after, right, columns):
    return pl.pallas_call(
        fetch_kernel,
        out_shape=jax.ShapeDtypeStruct((right.shape[0], columns), jnp.bfloat16),
        in_specs=[VMEM, HBM],
        out_specs=VMEM,
        scratch_shapes=[pltpu.SemaphoreType.DMA],
        compiler_params=pltpu.CompilerParams(vmem_limit_bytes=8 * MIB),
        name="fetch_columns",
    )(after, in_hbm(right))


def owners(table_ref, half):
    table = table_ref[half]
    return jnp.concatenate([table[col : col + 1] for col in range(table.shape[0])], axis=1)


def block_kernel(half, table_ref, *refs):
    parts = len(refs) - 10
    part_refs = refs[:parts]
    rows_ref, first_ref, right_hbm, left_hbm, out_ref, right_ref, left_ref, mixed_ref, shaped_ref, sem = refs[parts:]
    block_size = right_hbm.shape[0]
    tile = first_ref.shape[1]
    loads = start_loads(right_hbm, left_hbm, right_ref, left_ref, tile, sem)
    totals = part_refs[0][...]
    for part_ref in part_refs[1:]:
        totals = totals + part_ref[...]
    adam_sq = jnp.sum(jnp.where(owners(table_ref, half) == lax.axis_index(DP), totals, 0.0))
    places = [spread(slot) for slot in range(lax.axis_size(DP))]
    mix(rows_ref, first_ref, right_ref, mixed_ref, tile, loads, places)

    def shape(j, squares):
        cols = pl.ds(pl.multiple_of(j * tile, tile), tile)
        shaped = jnp.dot(left_ref[...], mixed_ref[:, cols], preferred_element_type=jnp.float32)
        shaped_ref[:, cols] = shaped
        return squares + jnp.sum((shaped * shaped).reshape(block_size // 8, 8, tile), axis=0)

    squares = lax.fori_loop(0, block_size // tile, shape, jnp.zeros((8, tile), jnp.float32))
    shaped_sq = jnp.full((8, 128), jnp.sum(squares), jnp.float32)
    scale = jnp.sqrt((adam_sq + NORM_EPS) / (shaped_sq + NORM_EPS))[0:1, 0:1]
    each = block_size // len(places)
    for group, place in enumerate(places):
        rows = shaped_ref[pl.ds(group * each, each), :] * scale
        out_ref[pl.ds(place * each, each), :] = rows.astype(jnp.bfloat16)


def raw_block_kernel(
    half, table_ref, rows_ref, first_ref, right_hbm, left_hbm, out_hbm, square_ref, right_ref, left_ref, mixed_ref, held_ref, sem
):
    block_size = right_hbm.shape[0]
    tile = first_ref.shape[1]
    steps = block_size // tile
    loads = start_loads(right_hbm, left_hbm, right_ref, left_ref, tile, sem)
    mix(rows_ref, first_ref, right_ref, mixed_ref, tile, loads)

    def store(j):
        cols = pl.ds(pl.multiple_of(j * tile, tile), tile)
        return pltpu.make_async_copy(held_ref.at[:, cols], out_hbm.at[:, cols], sem.at[j])

    def shape(j, squares):
        cols = pl.ds(pl.multiple_of(j * tile, tile), tile)
        shaped = jnp.dot(left_ref[...], mixed_ref[:, cols], preferred_element_type=jnp.float32)
        held_ref[:, cols] = shaped.astype(jnp.bfloat16)
        store(j).start()
        return squares + jnp.sum((shaped * shaped).reshape(block_size // 8, 8, tile), axis=0)

    squares = lax.fori_loop(0, steps, shape, jnp.zeros((8, tile), jnp.float32))
    square_ref[...] = jnp.where(owners(table_ref, half) == lax.axis_index(DP), jnp.sum(squares), 0.0)
    for j in range(steps):
        store(j).wait()


def start_loads(right_hbm, left_hbm, right_ref, left_ref, tile, sem):
    rest = pl.ds(tile, right_hbm.shape[1] - tile)
    right_load = pltpu.make_async_copy(right_hbm.at[:, rest], right_ref.at[:, rest], sem.at[0])
    left_load = pltpu.make_async_copy(left_hbm, left_ref, sem.at[1])
    right_load.start()
    left_load.start()
    return right_load, left_load


def mix(rows_ref, first_ref, right_ref, mixed_ref, tile, loads, places=None):
    for start in range(0, mixed_ref.shape[1], tile):
        cols = pl.ds(start, tile)
        if start == tile:
            loads[0].wait()
        columns = right_ref[:, cols] if start > 0 else first_ref[...]
        mixed = jnp.dot(rows_ref[...], columns, preferred_element_type=jnp.float32)
        mixed = mixed.astype(jnp.bfloat16)
        if places is None:
            mixed_ref[:, cols] = mixed
        else:
            each = mixed.shape[0] // len(places)
            for group, place in enumerate(places):
                mixed_ref[pl.ds(group * each, each), cols] = mixed[place * each : (place + 1) * each]
    loads[1].wait()


def own_block(rows_in, first, right, left, table, half, parts=()):
    block_size = right.shape[0]
    shape = (block_size, block_size)
    square = pltpu.VMEM(shape, jnp.bfloat16)
    finished = len(parts) > 0
    if finished:
        kernel, held = block_kernel, pltpu.VMEM(shape, jnp.float32)
        out_shape = jax.ShapeDtypeStruct(shape, jnp.bfloat16)
    else:
        kernel, held = raw_block_kernel, square
        out_shape = (pltpu.HBM(shape, jnp.bfloat16), jax.ShapeDtypeStruct((1, table[0].size), jnp.float32))
    return pl.pallas_call(
        functools.partial(kernel, half),
        out_shape=out_shape,
        in_specs=[VMEM] * (len(parts) + 3) + [HBM] * 2,
        out_specs=VMEM if finished else (HBM, VMEM),
        scratch_shapes=[square, square, square, held, pltpu.SemaphoreType.DMA((2,))],
        compiler_params=pltpu.CompilerParams(vmem_limit_bytes=24 * MIB),
        name="own_block" if finished else "raw_block",
        cost_estimate=pl.CostEstimate(
            flops=4 * block_size**3, bytes_accessed=8 * block_size**2, transcendentals=0
        ),
    )(table, *parts, rows_in, first, in_hbm(right), in_hbm(left))


def exchange(value, axes=DP):
    return lax.all_to_all(value, axes, split_axis=0, concat_axis=0, tiled=True)


def adam_sums(grad, second_moment, block_size):
    row_blocks, block_rows, half_cols = grad.shape
    col_blocks = half_cols // block_size
    widened = grad.astype(jnp.float32)
    square = widened * widened
    moment_new = BETA_TWO * second_moment + (1.0 - BETA_TWO) * square
    root = moment_new * lax.rsqrt(moment_new)
    ratio = square / (moment_new + ADAM_EPS * (2.0 * root + ADAM_EPS))
    sums = jnp.sum(ratio.reshape(row_blocks, block_rows, col_blocks, block_size), axis=(1, 3))
    return jnp.transpose(sums).reshape(1, row_blocks * col_blocks)


def plane_sums(value):
    return lax.psum(lax.psum(value, "dp_0"), "dp_2")


def all_shifts(value, axis):
    size = lax.axis_size(axis)
    values = [value]
    for step in range(1, size):
        ring = [(i, (i + step) % size) for i in range(size)]
        values.append(lax.ppermute(value, axis, ring))
    return values


def all_planes(plane):
    return all_shifts(plane, Z)


def first_core(grad, second_moment, left, right, table):
    block_size = left.shape[0]
    slots = lax.axis_size(DP)
    outgoing, first = gather_rows(table, grad, 1, slots, block_size, right)
    rows_in = exchange(outgoing)
    result, square = own_block(
        rows_in.reshape(block_size, block_size), first, right, left, table, 1
    )
    second_moment, result = lax.optimization_barrier((second_moment, result))
    back = exchange(result.reshape(outgoing.shape))
    sums = jnp.concatenate([adam_sums(grad, second_moment, block_size), square], axis=0)
    return scatter_rows(table, back, 1, grad, all_planes(plane_sums(sums)))


def second_core(grad, second_moment, left, right, table):
    block_size = left.shape[0]
    outgoing = gather_rows(table, grad, 0, lax.axis_size(DP), block_size)
    sums = sum(all_shifts(adam_sums(grad, second_moment, block_size), "dp_0"))
    parts = all_planes(sum(all_shifts(sums, "dp_2")))
    first = fetch_columns(parts[0], right, block_size // 2)
    first, *parts[:1], outgoing = lax.optimization_barrier((first, *parts[:1], outgoing))
    rows_in = exchange(outgoing, SPREAD)
    result = own_block(
        rows_in.reshape(block_size, block_size), first, right, left, table, 0, parts
    )
    back = exchange(result.reshape(outgoing.shape), SPREAD)
    return scatter_rows(table, back, 0, grad)


def per_device(grad, second_moment, left_root, right_root, owner_slot):
    table = jnp.transpose(owner_slot, (0, 2, 1))
    return lax.cond(
        lax.axis_index("mp") == 1,
        first_core,
        second_core,
        grad,
        second_moment,
        left_root[0, 0],
        right_root[0, 0],
        table,
    )


def solution(mesh):
    split = Mesh(mesh.devices.reshape(4, 2, 2, 2, 4, mesh.shape["mp"]), ("dp_0", *Z, "dp_2", "mp"))
    return jax.shard_map(
        per_device,
        mesh=split,
        in_specs=(
            P(None, DP, "mp"),
            P(None, DP, "mp"),
            P("mp", DP, None, None),
            P("mp", DP, None, None),
            P(),
        ),
        out_specs=P(None, DP, "mp"),
        check_vma=False,
    )
```
